256 devices in a mesh: fsdp: 32 (over z, y), ep: 8 (over x, core).
Axes of the slice: x: 4, y: 4, z: 8, core: 2. Of those that a mesh axis runs over, the one named last changes fastest.
Arguments:
- x_tok: bfloat16 [65536, 768], P(('fsdp', 'ep'))
- dy_tok: bfloat16 [65536, 768], P(('fsdp', 'ep'))
- expert_ids: int32 [65536, 2], P(('fsdp', 'ep'))
- route_w: float32 [65536, 2], P(('fsdp', 'ep'))
- w_gate: bfloat16 [8, 768, 2048], P('ep', 'fsdp')
- w_up: bfloat16 [8, 768, 2048], P('ep', 'fsdp')
- w_down: bfloat16 [8, 2048, 768], P('ep', None, 'fsdp')
Outputs:
- output 1: bfloat16 [65536, 768], P(('fsdp', 'ep'))
- output 2: float32 [65536, 2], P(('fsdp', 'ep'))
- output 3: float32 [8, 768, 2048], P('ep', 'fsdp')
- output 4: float32 [8, 768, 2048], P('ep', 'fsdp')
- output 5: float32 [8, 2048, 768], P('ep', None, 'fsdp')
All inputs are finite; a program needn't handle non-finite values.
Results may differ from the reference program's by a relative error of at most 0.00122.
Values are sent between devices in bfloat16 or wider.
A program may use at most 768 MiB of HBM per device.

```python
import jax
import jax.numpy as jnp
from jax import lax

D_MODEL = 768
D_FF = 2048
EXPERTS = 8
TOP_K = 2
TOK_DEV = 256
DEVICES = 256
CAPACITY = 192

TOKENS = DEVICES * TOK_DEV
SLOTS = EXPERTS * CAPACITY
HOT_COUNT = max(1, TOP_K // 2)


def draw_routing(root_key):
    key_hot, key_score = jax.random.split(root_key)
    hot_rank = jax.random.permutation(key_hot, EXPERTS)
    bias = jnp.where(hot_rank < HOT_COUNT, 768, 0).astype(jnp.int32)
    expert_col = jnp.arange(EXPERTS, dtype=jnp.int32)

    def one_device(dev_key):
        noise = jax.random.randint(dev_key, (TOK_DEV, EXPERTS), 0, 1024, dtype=jnp.int32)
        score = (noise + bias[None, :]) * EXPERTS + expert_col[None, :]
        return lax.top_k(score, TOP_K)[1]

    chosen = lax.map(one_device, jax.random.split(key_score, DEVICES))
    return chosen.reshape(TOKENS, TOP_K).astype(jnp.int32)


def setup_inputs(seed: int = 0) -> dict:
    key_list = jax.random.split(jax.random.key(seed), 7)
    x_tok = jax.random.normal(key_list[0], (TOKENS, D_MODEL), jnp.float32)
    dy_tok = jax.random.normal(key_list[1], (TOKENS, D_MODEL), jnp.float32)
    expert_ids = draw_routing(key_list[2])
    route_w = jax.random.uniform(key_list[3], (TOKENS, TOP_K), jnp.float32, 0.1, 1.0)
    w_gate = jax.random.normal(key_list[4], (EXPERTS, D_MODEL, D_FF), jnp.float32) * D_MODEL ** -0.5
    w_up = jax.random.normal(key_list[5], (EXPERTS, D_MODEL, D_FF), jnp.float32) * D_MODEL ** -0.5
    w_down = jax.random.normal(key_list[6], (EXPERTS, D_FF, D_MODEL), jnp.float32) * D_FF ** -0.5
    return {
        "x_tok": x_tok.astype(jnp.bfloat16),
        "dy_tok": dy_tok.astype(jnp.bfloat16),
        "expert_ids": expert_ids,
        "route_w": route_w,
        "w_gate": w_gate.astype(jnp.bfloat16),
        "w_up": w_up.astype(jnp.bfloat16),
        "w_down": w_down.astype(jnp.bfloat16),
    }


def slot_positions(ids_dev):
    onehot = (ids_dev[:, None] == jnp.arange(EXPERTS, dtype=jnp.int32)[None, :]).astype(jnp.int32)
    before = jnp.cumsum(onehot, axis=0) - onehot
    position = jnp.sum(before * onehot, axis=1)
    return jnp.where(position < CAPACITY, ids_dev * CAPACITY + position, SLOTS)


def swiglu_grads(pre_gate, pre_up, grad_hidden):
    sigma = jax.nn.sigmoid(pre_gate)
    grad_gate = grad_hidden * pre_up * sigma * (1.0 + pre_gate * (1.0 - sigma))
    grad_up = grad_hidden * pre_gate * sigma
    return grad_gate.astype(jnp.bfloat16), grad_up.astype(jnp.bfloat16)


def reference(x_tok, dy_tok, expert_ids, route_w, w_gate, w_up, w_down):
    dest_slot = lax.map(slot_positions, expert_ids.reshape(DEVICES, TOK_DEV * TOP_K))
    pair_ids = jnp.arange(TOKENS * TOP_K, dtype=jnp.int32).reshape(DEVICES, TOK_DEV * TOP_K)
    dev_rows = jnp.broadcast_to(jnp.arange(DEVICES, dtype=jnp.int32)[:, None], dest_slot.shape)
    slot_src = jnp.full((DEVICES, SLOTS + 1), TOKENS * TOP_K, jnp.int32)
    slot_src = slot_src.at[dev_rows, dest_slot].set(pair_ids)[:, :SLOTS]
    per_expert = slot_src.reshape(DEVICES, EXPERTS, CAPACITY).transpose(1, 0, 2).reshape(EXPERTS, DEVICES * CAPACITY)
    route_flat = route_w.reshape(-1)

    def expert_step(carry, step_in):
        dx_acc, dr_acc = carry
        pair_src, w_gate_e, w_up_e, w_down_e = step_in
        tok_rows = pair_src // TOP_K
        x_rows = jnp.take(x_tok, tok_rows, axis=0, mode="fill", fill_value=0)
        dy_rows = jnp.take(dy_tok, tok_rows, axis=0, mode="fill", fill_value=0)
        gate_rows = jnp.take(route_flat, pair_src, axis=0, mode="fill", fill_value=0)
        pre_gate = jnp.dot(x_rows, w_gate_e, preferred_element_type=jnp.float32)
        pre_up = jnp.dot(x_rows, w_up_e, preferred_element_type=jnp.float32)
        hidden = (jax.nn.silu(pre_gate) * pre_up).astype(jnp.bfloat16)
        y_rows = jnp.dot(hidden, w_down_e, preferred_element_type=jnp.float32)
        dy_wide = dy_rows.astype(jnp.float32)
        scaled_dy = (gate_rows[:, None] * dy_wide).astype(jnp.bfloat16)
        dr_rows = jnp.sum(dy_wide * y_rows, axis=1)
        grad_hidden = jnp.dot(scaled_dy, w_down_e.T, preferred_element_type=jnp.float32)
        grad_gate, grad_up = swiglu_grads(pre_gate, pre_up, grad_hidden)
        dx_rows = (jnp.dot(grad_gate, w_gate_e.T, preferred_element_type=jnp.float32)
                   + jnp.dot(grad_up, w_up_e.T, preferred_element_type=jnp.float32)).astype(jnp.bfloat16)
        dw_gate = jnp.dot(x_rows.T, grad_gate, preferred_element_type=jnp.float32)
        dw_up = jnp.dot(x_rows.T, grad_up, preferred_element_type=jnp.float32)
        dw_down = jnp.dot(hidden.T, scaled_dy, preferred_element_type=jnp.float32)
        dx_acc = dx_acc.at[tok_rows].add(dx_rows.astype(jnp.float32), mode="drop")
        dr_acc = dr_acc.at[pair_src].set(dr_rows, mode="drop")
        return (dx_acc, dr_acc), (dw_gate, dw_up, dw_down)

    init = (jnp.zeros((TOKENS, D_MODEL), jnp.float32), jnp.zeros((TOKENS * TOP_K,), jnp.float32))
    (dx_acc, dr_acc), (grad_w_gate, grad_w_up, grad_w_down) = lax.scan(
        expert_step, init, (per_expert, w_gate, w_up, w_down))
    grad_x = dx_acc.astype(jnp.bfloat16)
    route_w_grad = dr_acc.reshape(TOKENS, TOP_K)
    return (grad_x, route_w_grad, grad_w_gate, grad_w_up, grad_w_down)
```

```python
import jax
import jax.numpy as jnp
from jax import lax
from jax.experimental import pallas as pl
from jax.experimental.pallas import tpu as pltpu
from jax.sharding import PartitionSpec as P

CAP_FACTOR = 3
MESH = pl.DeviceIdType.MESH
NZ, NY, NX = 8, 4, 4
RING = NZ * NY
HALF = RING // 2
PEERS = 8


def capacity_of(tok_dev, top_k, experts):
    return max(8, ((CAP_FACTOR * tok_dev * top_k // experts + 7) // 8) * 8)


def ring_pos(k, i):
    z, y = lax.div(i, NY), lax.rem(i, NY)
    if k == 0:
        return z * NY + lax.rem(y + z, NY)
    o = lax.rem(z - 3 * y + 16, NZ)
    return NY * y + lax.rem(o, NY) + HALF * lax.div(o, NY)


def ring_dev(k, p):
    p = lax.rem(p + 2 * RING, RING)
    a, b = lax.div(p, NY), lax.rem(p, NY)
    if k == 0:
        z, y = a, lax.rem(b - a + 8, NY)
    else:
        z, y = lax.rem(3 * a + b, NZ), lax.rem(a, NY)
    return z * NY + y


def signal_all(targets):
    barrier = pltpu.get_barrier_semaphore()
    for t in targets:
        pl.semaphore_signal(barrier, inc=1, device_id=t, device_id_type=MESH)
    pl.semaphore_wait(barrier, len(targets))


def ds128(start, size):
    return pl.ds(start, size)


def gather_kernel(x_ref, dy_ref, meta_ref, w_ref, xall, dyall, metaall, wall,
                  loc_sem, wsend, wrecv, tsend, trecv):
    i, p = lax.axis_index("fsdp"), lax.axis_index("ep")
    chip, core = lax.div(p, 2), lax.rem(p, 2)
    xr = lax.rem(chip + 1, NX) * 2 + core
    xl = lax.rem(chip + NX - 1, NX) * 2 + core
    xo = lax.rem(chip + 2, NX) * 2 + core
    partner = chip * 2 + 1 - core
    pos = [ring_pos(k, i) for k in (0, 1)]
    hop = [[ring_dev(k, pos[k] + 1), ring_dev(k, pos[k] - 1)] for k in (0, 1)]
    signal_all([{"fsdp": hop[k][d]} for k in (0, 1) for d in (0, 1)] + [{"ep": e} for e in (xr, xl, partner)])

    width = w_ref.shape[-1]
    nsub = wsend.shape[2]
    cols = width // (2 * nsub)

    own = [pltpu.make_async_copy(s, d, loc_sem.at[n]) for n, (s, d) in enumerate(
        ((x_ref, xall.at[p]), (dy_ref, dyall.at[p]), (meta_ref, metaall.at[p]), (w_ref, wall.at[:, i])))]
    for c in own:
        c.start()

    def wcopy(s, k, d, u, src=None):
        t = ring_dev(k, pos[k] - s if d == 0 else pos[k] + s)
        sl = pl.ds(k * (width // 2) + u * cols, cols)
        dst = wall.at[:, t, :, sl]
        return pltpu.make_async_remote_copy(
            src_ref=w_ref.at[:, :, sl] if src is None else dst, dst_ref=dst,
            send_sem=wsend.at[k, d, u], recv_sem=wrecv.at[s, k, d, u],
            device_id={"fsdp": hop[k][d]}, device_id_type=MESH)

    def tcopy(n, which, block, to, own_block=False):
        src, dst = ((x_ref, xall), (dy_ref, dyall), (meta_ref, metaall))[which]
        return pltpu.make_async_remote_copy(
            src_ref=src if own_block else dst.at[block], dst_ref=dst.at[block],
            send_sem=tsend.at[n], recv_sem=trecv.at[n],
            device_id={"ep": to}, device_id_type=MESH)

    subs = [(k, d, u) for u in range(nsub) for k in (0, 1) for d in (0, 1)]
    for k, d, u in subs:
        wcopy(0, k, d, u).start()
    first = [tcopy(3 * r + w, w, p, to, True) for r, to in ((0, xr), (1, xl), (2, partner)) for w in (2, 0, 1)]
    for c in first:
        c.start()

    def step(s):
        for k, d, u in subs:
            wcopy(s - 1, k, d, u, 1).wait_recv()
            wcopy(s - 1, k, d, u, 1).wait_send()
            wcopy(s, k, d, u, 1).start()

    def run(lo, hi):
        def body(s, c):
            step(s)
            return c
        lax.fori_loop(lo, hi, body, 0)

    run(1, 6)
    second, fwd = [], []
    for r, src in ((0, xl), (1, xr)):
        for w in (2, 0, 1):
            tcopy(3 * r + w, w, src, xr).wait_recv()
    for n, w, src, to in ((18 + 2, 2, xl, xr), (18 + 1, 1, xl, xr), (18 + 0, 0, xr, xl)):
        second.append(tcopy(n, w, src, to))
        second[-1].start()
    for r, src in ((3, xl), (4, xr)):
        for w in (2, 0, 1):
            fwd.append(tcopy(3 * r + w, w, src, partner))
            fwd[-1].start()
    run(6, 11)
    for n, w in ((18 + 2, 2), (18 + 1, 1), (18 + 0, 0)):
        tcopy(n, w, xo, xr).wait_recv()
    for w in (2, 0, 1):
        fwd.append(tcopy(15 + w, w, xo, partner))
        fwd[-1].start()
    run(11, HALF - 1)
    for k, d, u in subs:
        wcopy(HALF - 2, k, d, u, 1).wait_recv()
        wcopy(HALF - 2, k, d, u, 1).wait_send()
        if d == 0:
            wcopy(HALF - 1, k, d, u, 1).start()
    for c in first + second + fwd:
        c.wait_send()
    xpr, xpl = lax.rem(chip + 1, NX) * 2 + 1 - core, lax.rem(chip + NX - 1, NX) * 2 + 1 - core
    xpo = lax.rem(chip + 2, NX) * 2 + 1 - core
    for r, src in ((2, partner), (3, xpl), (4, xpr), (5, xpo)):
        for w in (2, 0, 1):
            tcopy(3 * r + w, w, src, partner).wait_recv()
    for c in own:
        c.wait()
    for k, d, u in subs:
        if d == 0:
            wcopy(HALF - 1, k, d, u, 1).wait_recv()
            wcopy(HALF - 1, k, d, u, 1).wait_send()


def gather_all(x_tok, dy_tok, meta, w):
    nsub = 4
    n3, rows, width = w.shape
    return pl.pallas_call(
        gather_kernel,
        out_shape=(jax.ShapeDtypeStruct((PEERS, *x_tok.shape), x_tok.dtype),
                   jax.ShapeDtypeStruct((PEERS, *dy_tok.shape), dy_tok.dtype),
                   jax.ShapeDtypeStruct((PEERS, *meta.shape), meta.dtype),
                   jax.ShapeDtypeStruct((n3, RING, rows, width), w.dtype)),
        in_specs=[pl.BlockSpec(memory_space=pltpu.VMEM)] * 4,
        out_specs=[pl.BlockSpec(memory_space=pltpu.VMEM)] * 4,
        scratch_shapes=[
            pltpu.SemaphoreType.DMA((4,)),
            pltpu.SemaphoreType.DMA((2, 2, nsub)),
            pltpu.SemaphoreType.DMA((HALF, 2, 2, nsub)),
            pltpu.SemaphoreType.DMA((21,)),
            pltpu.SemaphoreType.DMA((21,)),
        ],
        compiler_params=pltpu.CompilerParams(
            collective_id=0, has_side_effects=True, vmem_limit_bytes=60000 * 1024),
        name="gather_all",
    )(x_tok, dy_tok, meta, w)


def scatter_kernel(dx_ref, dr_ref, g0_ref, g1_ref, g2_ref, dx_out, dr_out, g_out,
                   up, down, loc_sem, xsend, xrecv, gsend, grecv):
    i, p = lax.axis_index("fsdp"), lax.axis_index("ep")
    pos = [ring_pos(k, i) for k in (0, 1)]
    hop = [[ring_dev(k, pos[k] + 1), ring_dev(k, pos[k] - 1)] for k in (0, 1)]
    peer = [lax.rem(p + r, PEERS) for r in range(1, PEERS)]
    signal_all([{"fsdp": hop[k][d]} for k in (0, 1) for d in (0, 1)] + [{"ep": e} for e in peer])

    width = g_out.shape[-1]
    nsub = gsend.shape[2]
    cols = width // (2 * nsub)
    slots = (up, down)
    grads = (g0_ref, g1_ref, g2_ref)
    subs = [(k, d, u) for u in range(nsub) for k in (0, 1) for d in (0, 1)]

    def gcopy(s, k, d, u):
        sl = pl.ds(k * (width // 2) + u * cols, cols)
        return pltpu.make_async_remote_copy(
            src_ref=slots[d].at[s, :, :, sl], dst_ref=slots[d].at[s + 1, :, :, sl],
            send_sem=gsend.at[k, d, u], recv_sem=grecv.at[s, k, d, u],
            device_id={"fsdp": hop[k][d]}, device_id_type=MESH)

    def add_local(s, k, d, u, fresh):
        t = ring_dev(k, pos[k] + HALF - s if d == 0 else pos[k] - (HALF - 1) + s)
        sl = pl.ds(k * (width // 2) + u * cols, cols)
        for n in range(3):
            mine = grads[n][t, :, sl]
            slots[d][s, n, :, sl] = mine if fresh else slots[d][s, n, :, sl] + mine

    for k, d, u in subs:
        add_local(0, k, d, u, True)
        gcopy(0, k, d, u).start()

    own = [pltpu.make_async_copy(dx_ref.at[p], dx_out.at[p], loc_sem.at[0]),
           pltpu.make_async_copy(dr_ref.at[p], dr_out.at[p], loc_sem.at[1])]
    for c in own:
        c.start()

    def xcopy(r, which, dst_peer, slot):
        src, dst = ((dx_ref, dx_out), (dr_ref, dr_out))[which]
        return pltpu.make_async_remote_copy(
            src_ref=src.at[dst_peer], dst_ref=dst.at[slot],
            send_sem=xsend.at[r, which], recv_sem=xrecv.at[r, which],
            device_id={"ep": dst_peer}, device_id_type=MESH)

    sent = [xcopy(r, w, peer[r], p) for r in range(PEERS - 1) for w in (0, 1)]
    for c in sent:
        c.start()

    def body(s, c):
        for k, d, u in subs:
            gcopy(s - 1, k, d, u).wait_recv()
            gcopy(s - 1, k, d, u).wait_send()
            add_local(s, k, d, u, False)
            gcopy(s, k, d, u).start()
        return c
    lax.fori_loop(1, HALF - 1, body, 0)
    for k, d, u in subs:
        gcopy(HALF - 2, k, d, u).wait_recv()
        gcopy(HALF - 2, k, d, u).wait_send()
        if d == 0:
            add_local(HALF - 1, k, d, u, False)
            gcopy(HALF - 1, k, d, u).start()
    for c in sent:
        c.wait_send()
    for r in range(PEERS - 1):
        for w in (0, 1):
            xcopy(r, w, peer[r], lax.rem(p + PEERS - 1 - r, PEERS)).wait_recv()
    for c in own:
        c.wait()
    for k, d, u in subs:
        if d == 0:
            gcopy(HALF - 1, k, d, u).wait_recv()
            gcopy(HALF - 1, k, d, u).wait_send()
            sl = pl.ds(k * (width // 2) + u * cols, cols)
            for n in range(3):
                g_out[n, :, sl] = up[HALF, n, :, sl] + down[HALF - 1, n, :, sl] + grads[n][i, :, sl]


def scatter_all(dx, dr, g0, g1, g2):
    nsub = 2
    _, rows, width = g0.shape
    f32 = jnp.float32
    return pl.pallas_call(
        scatter_kernel,
        out_shape=(jax.ShapeDtypeStruct(dx.shape, dx.dtype), jax.ShapeDtypeStruct(dr.shape, dr.dtype),
                   jax.ShapeDtypeStruct((3, rows, width), f32)),
        in_specs=[pl.BlockSpec(memory_space=pltpu.VMEM)] * 5,
        out_specs=[pl.BlockSpec(memory_space=pltpu.VMEM)] * 3,
        scratch_shapes=[
            pltpu.VMEM((HALF + 1, 3, rows, width), f32),
            pltpu.VMEM((HALF, 3, rows, width), f32),
            pltpu.SemaphoreType.DMA((2,)),
            pltpu.SemaphoreType.DMA((PEERS - 1, 2)),
            pltpu.SemaphoreType.DMA((PEERS - 1, 2)),
            pltpu.SemaphoreType.DMA((2, 2, nsub)),
            pltpu.SemaphoreType.DMA((HALF, 2, 2, nsub)),
        ],
        compiler_params=pltpu.CompilerParams(
            collective_id=1, has_side_effects=True, vmem_limit_bytes=60000 * 1024),
        name="scatter_all",
    )(dx, dr, g0, g1, g2)


def mm(a, b, dims):
    return lax.dot_general(a, b, (dims, ((), ())), preferred_element_type=jnp.float32)


def solution(mesh):
    tok_spec = P(("fsdp", "ep"), None)
    spec_in = P("ep", "fsdp", None)
    spec_out = P("ep", None, "fsdp")

    def per_device(x_tok, dy_tok, expert_ids, route_w, w_gate, w_up, w_down):
        tok_dev, top_k = expert_ids.shape
        d_model = x_tok.shape[1]
        d_ff = w_gate.shape[2]
        capacity = capacity_of(tok_dev, top_k, PEERS)
        me = lax.axis_index("ep")
        f32, bf16 = jnp.float32, jnp.bfloat16
        meta = jnp.concatenate([expert_ids.T.astype(f32), route_w.T, jnp.zeros((4, tok_dev), f32)], axis=0)
        w_local = jnp.stack([w_gate[0], w_up[0], w_down[0].T])
        x_all, dy_all, meta_all, w_all = gather_all(x_tok, dy_tok, meta, w_local)

        ids_all = meta_all[:, 0:top_k]
        hit = ids_all == me.astype(f32)
        mine = jnp.any(hit, axis=1)
        count = mine.astype(jnp.int32)
        place = jnp.where(mine, jnp.cumsum(count, axis=1) - count, capacity)
        pick = place[:, None, :] == jnp.arange(capacity, dtype=jnp.int32)[None, :, None]
        weight = jnp.sum(jnp.where(hit, meta_all[:, top_k:2 * top_k], 0.0), axis=1)
        gate_rows = jnp.sum(jnp.where(pick, weight[:, None, :], 0.0), axis=2).reshape(-1)
        pick = pick.astype(bf16)
        x_rows = jnp.einsum("sct,std->scd", pick, x_all, preferred_element_type=f32).astype(bf16)
        dy_rows = jnp.einsum("sct,std->scd", pick, dy_all, preferred_element_type=f32).astype(bf16)
        x_rows, dy_rows = x_rows.reshape(-1, d_model), dy_rows.reshape(-1, d_model)

        w_all = w_all.reshape(3, d_model, d_ff)
        w1, w3, w2t = w_all[0], w_all[1], w_all[2]
        pre_gate = mm(x_rows, w1, ((1,), (0,)))
        pre_up = mm(x_rows, w3, ((1,), (0,)))
        hidden = (jax.nn.silu(pre_gate) * pre_up).astype(bf16)
        y_rows = mm(hidden, w2t, ((1,), (1,)))
        dy_wide = dy_rows.astype(f32)
        scaled_dy = (gate_rows[:, None] * dy_wide).astype(bf16)
        dr_rows = jnp.sum(dy_wide * y_rows, axis=-1)
        grad_hidden = mm(scaled_dy, w2t, ((1,), (0,)))
        sigma = jax.nn.sigmoid(pre_gate)
        dh1 = (grad_hidden * pre_up * sigma * (1.0 + pre_gate * (1.0 - sigma))).astype(bf16)
        dh3 = (grad_hidden * pre_gate * sigma).astype(bf16)
        dx_rows = (mm(dh1, w1, ((1,), (1,))) + mm(dh3, w3, ((1,), (1,)))).astype(bf16)
        dw1 = mm(x_rows, dh1, ((0,), (0,)))
        dw3 = mm(x_rows, dh3, ((0,), (0,)))
        dw2t = mm(scaled_dy, hidden, ((0,), (0,)))

        blocks = (RING, d_model // RING, d_ff)
        dr_pad = jnp.pad(dr_rows.reshape(PEERS, capacity), ((0, 0), (0, 1024 - capacity))).reshape(PEERS, 8, 128)
        dx_back, dr_back, g = scatter_all(
            dx_rows.reshape(PEERS, capacity, d_model), dr_pad,
            dw1.reshape(blocks), dw3.reshape(blocks), dw2t.reshape(blocks))

        onehot = expert_ids[:, :, None] == jnp.arange(PEERS, dtype=jnp.int32)
        used = jnp.any(onehot, axis=1).astype(jnp.int32)
        before = jnp.cumsum(used, axis=0) - used
        spot = jnp.sum(jnp.where(onehot, before[:, None, :], 0), axis=2)
        n_slots = PEERS * capacity
        slot = jnp.where(spot < capacity, expert_ids * capacity + spot, n_slots)
        at = slot[:, :, None] == jnp.arange(n_slots, dtype=jnp.int32)
        dr_flat = dr_back.reshape(PEERS, 1024)[:, :capacity].reshape(-1)
        route_grad = jnp.sum(jnp.where(at, dr_flat, 0.0), axis=2)
        grad_x = mm(jnp.any(at, axis=1).astype(bf16), dx_back.reshape(n_slots, d_model), ((1,), (0,))).astype(bf16)
        return grad_x, route_grad, g[0][None], g[1][None], g[2].T[None]

    return jax.shard_map(
        per_device, mesh=mesh,
        in_specs=(tok_spec, tok_spec, tok_spec, tok_spec, spec_in, spec_in, spec_out),
        out_specs=(tok_spec, tok_spec, spec_in, spec_in, spec_out),
        check_vma=False)
```

```python
import jax
import jax.numpy as jnp
from jax import lax
from jax.experimental import pallas as pl
from jax.experimental.pallas import tpu as pltpu
from jax.sharding import PartitionSpec as P

CAP_FACTOR = 3
MESH = pl.DeviceIdType.MESH
NZ, NY, NX = 8, 4, 4
RING = NZ * NY
HALF = RING // 2
PEERS = 8


def capacity_of(tok_dev, top_k, experts):
    return max(8, ((CAP_FACTOR * tok_dev * top_k // experts + 7) // 8) * 8)


def ring_pos(k, i):
    z, y = lax.div(i, NY), lax.rem(i, NY)
    if k == 0:
        return z * NY + lax.rem(y + z, NY)
    o = lax.rem(z - 3 * y + 16, NZ)
    return NY * y + lax.rem(o, NY) + HALF * lax.div(o, NY)


def ring_dev(k, p):
    p = lax.rem(p + 2 * RING, RING)
    a, b = lax.div(p, NY), lax.rem(p, NY)
    if k == 0:
        z, y = a, lax.rem(b - a + 8, NY)
    else:
        z, y = lax.rem(3 * a + b, NZ), lax.rem(a, NY)
    return z * NY + y


def signal_all(targets):
    barrier = pltpu.get_barrier_semaphore()
    for t in targets:
        pl.semaphore_signal(barrier, inc=1, device_id=t, device_id_type=MESH)
    pl.semaphore_wait(barrier, len(targets))


def gather_kernel(x_ref, dy_ref, meta_ref, w_ref, xall, dyall, metaall, wall,
                  loc_sem, wsend, wrecv, tsend, trecv):
    i, p = lax.axis_index("fsdp"), lax.axis_index("ep")
    chip, core = lax.div(p, 2), lax.rem(p, 2)
    xr = lax.rem(chip + 1, NX) * 2 + core
    xl = lax.rem(chip + NX - 1, NX) * 2 + core
    xo = lax.rem(chip + 2, NX) * 2 + core
    partner = chip * 2 + 1 - core
    pos = [ring_pos(k, i) for k in (0, 1)]
    hop = [[ring_dev(k, pos[k] + 1), ring_dev(k, pos[k] - 1)] for k in (0, 1)]
    signal_all([{"fsdp": hop[k][d]} for k in (0, 1) for d in (0, 1)] + [{"ep": e} for e in (xr, xl, partner)])

    width = w_ref.shape[-1]
    nsub = wsend.shape[2]
    cols = width // (2 * nsub)

    own = [pltpu.make_async_copy(s, d, loc_sem.at[n]) for n, (s, d) in enumerate(
        ((x_ref, xall.at[p]), (dy_ref, dyall.at[p]), (meta_ref, metaall.at[p]), (w_ref, wall.at[:, i])))]
    for c in own:
        c.start()

    def wcopy(s, k, d, u, src=None):
        t = ring_dev(k, pos[k] - s if d == 0 else pos[k] + s)
        sl = pl.ds(k * (width // 2) + u * cols, cols)
        dst = wall.at[:, t, :, sl]
        return pltpu.make_async_remote_copy(
            src_ref=w_ref.at[:, :, sl] if src is None else dst, dst_ref=dst,
            send_sem=wsend.at[k, d, u], recv_sem=wrecv.at[s, k, d, u],
            device_id={"fsdp": hop[k][d]}, device_id_type=MESH)

    def tcopy(n, which, block, to, own_block=False):
        src, dst = ((x_ref, xall), (dy_ref, dyall), (meta_ref, metaall))[which]
        return pltpu.make_async_remote_copy(
            src_ref=src if own_block else dst.at[block], dst_ref=dst.at[block],
            send_sem=tsend.at[n], recv_sem=trecv.at[n],
            device_id={"ep": to}, device_id_type=MESH)

    subs = [(k, d, u) for u in range(nsub) for k in (0, 1) for d in (0, 1)]
    for k, d, u in subs:
        wcopy(0, k, d, u).start()
    first = [tcopy(3 * r + w, w, p, to, True) for r, to in ((0, xr), (1, xl), (2, partner)) for w in (2, 0, 1)]
    for c in first:
        c.start()

    def step(s):
        for k, d, u in subs:
            wcopy(s - 1, k, d, u, 1).wait_recv()
            wcopy(s - 1, k, d, u, 1).wait_send()
            wcopy(s, k, d, u, 1).start()

    def run(lo, hi):
        def body(s, c):
            step(s)
            return c
        lax.fori_loop(lo, hi, body, 0)

    run(1, 6)
    second, fwd = [], []
    for r, src in ((0, xl), (1, xr)):
        for w in (2, 0, 1):
            tcopy(3 * r + w, w, src, xr).wait_recv()
    for n, w, src, to in ((18 + 2, 2, xl, xr), (18 + 1, 1, xl, xr), (18 + 0, 0, xr, xl)):
        second.append(tcopy(n, w, src, to))
        second[-1].start()
    for r, src in ((3, xl), (4, xr)):
        for w in (2, 0, 1):
            fwd.append(tcopy(3 * r + w, w, src, partner))
            fwd[-1].start()
    run(6, 11)
    for n, w in ((18 + 2, 2), (18 + 1, 1), (18 + 0, 0)):
        tcopy(n, w, xo, xr).wait_recv()
    for w in (2, 0, 1):
        fwd.append(tcopy(15 + w, w, xo, partner))
        fwd[-1].start()
    run(11, HALF - 1)
    for k, d, u in subs:
        wcopy(HALF - 2, k, d, u, 1).wait_recv()
        wcopy(HALF - 2, k, d, u, 1).wait_send()
        if d == 0:
            wcopy(HALF - 1, k, d, u, 1).start()
    for c in first + second + fwd:
        c.wait_send()
    xpr, xpl = lax.rem(chip + 1, NX) * 2 + 1 - core, lax.rem(chip + NX - 1, NX) * 2 + 1 - core
    xpo = lax.rem(chip + 2, NX) * 2 + 1 - core
    for r, src in ((2, partner), (3, xpl), (4, xpr), (5, xpo)):
        for w in (2, 0, 1):
            tcopy(3 * r + w, w, src, partner).wait_recv()
    for c in own:
        c.wait()
    for k, d, u in subs:
        if d == 0:
            wcopy(HALF - 1, k, d, u, 1).wait_recv()
            wcopy(HALF - 1, k, d, u, 1).wait_send()


def gather_all(x_tok, dy_tok, meta, w):
    nsub = 4
    n3, rows, width = w.shape
    return pl.pallas_call(
        gather_kernel,
        out_shape=(jax.ShapeDtypeStruct((PEERS, *x_tok.shape), x_tok.dtype),
                   jax.ShapeDtypeStruct((PEERS, *dy_tok.shape), dy_tok.dtype),
                   jax.ShapeDtypeStruct((PEERS, *meta.shape), meta.dtype),
                   jax.ShapeDtypeStruct((n3, RING, rows, width), w.dtype)),
        in_specs=[pl.BlockSpec(memory_space=pltpu.VMEM)] * 4,
        out_specs=[pl.BlockSpec(memory_space=pltpu.VMEM)] * 4,
        scratch_shapes=[
            pltpu.SemaphoreType.DMA((4,)),
            pltpu.SemaphoreType.DMA((2, 2, nsub)),
            pltpu.SemaphoreType.DMA((HALF, 2, 2, nsub)),
            pltpu.SemaphoreType.DMA((21,)),
            pltpu.SemaphoreType.DMA((21,)),
        ],
        compiler_params=pltpu.CompilerParams(
            collective_id=0, has_side_effects=True, vmem_limit_bytes=60000 * 1024),
        name="gather_all",
    )(x_tok, dy_tok, meta, w)


CHUNK = 256
ROWS = 512


def dot(a, b, ca, cb):
    return lax.dot_general(a, b, (((ca,), (cb,)), ((), ())), preferred_element_type=jnp.float32)


def expert_kernel(x_ref, dy_ref, g_ref, w_hbm, dx_out, dr_out, g_out,
                  wbuf, dw, up, down, dx_acc, dx_send, dr_acc, dr_send,
                  w_sem, loc_sem, xsend, xrecv, gsend, grecv):
    f32, bf16 = jnp.float32, jnp.bfloat16
    i, p = lax.axis_index("fsdp"), lax.axis_index("ep")
    pos = [ring_pos(k, i) for k in (0, 1)]
    hop = [[ring_dev(k, pos[k] + 1), ring_dev(k, pos[k] - 1)] for k in (0, 1)]
    peer = [lax.rem(p + r, PEERS) for r in range(1, PEERS)]
    signal_all([{"fsdp": hop[k][d]} for k in (0, 1) for d in (0, 1)] + [{"ep": e} for e in peer])

    chunks = dw.shape[0]
    tiles = x_ref.shape[0] // ROWS
    block = up.shape[3]
    half = CHUNK // 2
    slots = (up, down)

    def wload(c):
        return pltpu.make_async_copy(
            w_hbm.at[:, :, pl.ds(pl.multiple_of(c * CHUNK, CHUNK), CHUNK)], wbuf.at[lax.rem(c, 2)],
            w_sem.at[lax.rem(c, 2)])

    def rows_of(k, t):
        return pl.ds(pl.multiple_of(ring_dev(k, t) * block, 8), block)

    def gcopy(c, s, k, d):
        t = pos[k] + HALF - s if d == 0 else pos[k] - (HALF - 1) + s
        sl = pl.ds(k * half, half)
        return pltpu.make_async_remote_copy(
            src_ref=dw.at[c, :, rows_of(k, t), sl], dst_ref=slots[d].at[c, s, :, :, sl],
            send_sem=gsend.at[c, k, d], recv_sem=grecv.at[c, s, k, d],
            device_id={"fsdp": hop[k][d]}, device_id_type=MESH)

    def advance(c, s, k, d):
        @pl.when(s >= 1)
        def _():
            gcopy(c, s - 1, k, d).wait_recv()
            gcopy(c, s - 1, k, d).wait_send()
            t = pos[k] + HALF - s if d == 0 else pos[k] - (HALF - 1) + s
            rows, sl = rows_of(k, t), pl.ds(k * half, half)
            for n in range(3):
                dw[c, n, rows, sl] = dw[c, n, rows, sl] + slots[d][c, s - 1, n, :, sl]
        gcopy(c, s, k, d).start()

    def serve(q):
        lo = lax.max(lax.div(q - HALF + tiles - 1 + tiles * chunks, tiles) - chunks - 1, 0)
        hi = lax.min(lax.div(q, tiles), chunks)

        def one(c, carry):
            s = q - (c + 1) * tiles

            @pl.when(s < HALF)
            def _():
                for k in (0, 1):
                    advance(c, s, k, 0)

                @pl.when(s >= 1)
                def _():
                    for k in (0, 1):
                        advance(c, s - 1, k, 1)

            @pl.when(s == HALF)
            def _():
                for k in (0, 1):
                    sl = pl.ds(k * half, half)
                    gcopy(c, HALF - 1, k, 0).wait_recv()
                    gcopy(c, HALF - 1, k, 0).wait_send()
                    gcopy(c, HALF - 2, k, 1).wait_recv()
                    gcopy(c, HALF - 2, k, 1).wait_send()
                    rows = pl.ds(pl.multiple_of(i * block, 8), block)
                    out = pl.ds(pl.multiple_of(c * CHUNK, CHUNK) + k * half, half)
                    for n in range(3):
                        g_out[n, :, out] = (dw[c, n, rows, sl] + up[c, HALF - 1, n, :, sl]
                                            + down[c, HALF - 2, n, :, sl])
            return carry
        lax.fori_loop(lo, hi, one, 0)

    def compute(c, r):
        w = wbuf.at[lax.rem(c, 2)]
        w1, w3, w2t = w[0], w[1], w[2]
        rows = pl.ds(pl.multiple_of(r * ROWS, ROWS), ROWS)
        x, dy, g = x_ref[rows, :], dy_ref[rows, :], g_ref[rows, :]
        h1, h3 = dot(x, w1, 1, 0), dot(x, w3, 1, 0)
        da, u = dot(g, w2t, 1, 0), dot(dy, w2t, 1, 0)
        s = jax.nn.sigmoid(h1)
        a = (h1 * s * h3).astype(bf16)
        dh1 = (da * h3 * s * (1.0 + h1 * (1.0 - s))).astype(bf16)
        dh3 = (da * h1 * s).astype(bf16)
        au = a.astype(f32) * u
        dr = au[:, :128] + au[:, 128:]
        dx = dot(dh1, w1, 1, 1) + dot(dh3, w3, 1, 1)

        @pl.when(c == 0)
        def _():
            dr_acc[rows, :] = dr
            dx_acc[rows, :] = dx

        @pl.when(c > 0)
        def _():
            dr_acc[rows, :] += dr
            dx_acc[rows, :] += dx

        for n, (l, m) in enumerate(((x, dh1), (x, dh3), (g, a))):
            t = dot(l, m, 0, 0)

            @pl.when(r == 0)
            def _():
                dw[c, n] = t

            @pl.when(r > 0)
            def _():
                dw[c, n] += t

    wload(0).start()

    def step(q, carry):
        c, r = lax.div(q, tiles), lax.rem(q, tiles)

        @pl.when(r == 0)
        def _():
            wload(c).wait()

            @pl.when(c + 1 < chunks)
            def _():
                wload(c + 1).start()
        compute(c, r)
        serve(q + 1)
        return carry
    lax.fori_loop(0, tiles * chunks, step, 0)

    dx_send[...] = dx_acc[...].astype(bf16).reshape(dx_send.shape)
    total = jnp.sum(jnp.transpose(dr_acc[...]), axis=0, keepdims=True)
    cap = dx_send.shape[1]
    for e in range(PEERS):
        dr_send[e, 0:1, 0:cap] = total[:, e * cap:(e + 1) * cap]

    pairs = ((dx_send, dx_out), (dr_send, dr_out))
    own = [pltpu.make_async_copy(s.at[p], d.at[p], loc_sem.at[n]) for n, (s, d) in enumerate(pairs)]

    def xcopy(r, which, dst_peer, slot):
        src, dst = pairs[which]
        return pltpu.make_async_remote_copy(
            src_ref=src.at[dst_peer], dst_ref=dst.at[slot],
            send_sem=xsend.at[r, which], recv_sem=xrecv.at[r, which],
            device_id={"ep": dst_peer}, device_id_type=MESH)

    sent = [xcopy(r, w, peer[r], p) for r in range(PEERS - 1) for w in (0, 1)]
    for c in own + sent:
        c.start()

    def tail(q, carry):
        serve(q)
        return carry
    lax.fori_loop(tiles * chunks + 1, tiles * chunks + HALF + 1, tail, 0)

    for c in sent:
        c.wait_send()
    for r in range(PEERS - 1):
        for w in (0, 1):
            xcopy(r, w, peer[r], lax.rem(p + PEERS - 1 - r, PEERS)).wait_recv()
    for c in own:
        c.wait()


def expert_step(x, dy, g, w, capacity):
    n_rows, d_model = x.shape
    width = w.shape[2]
    block, chunks = d_model // RING, width // CHUNK
    f32, bf16 = jnp.float32, jnp.bfloat16
    vmem = pl.BlockSpec(memory_space=pltpu.VMEM)
    hbm = pl.BlockSpec(memory_space=pl.ANY)
    dma = pltpu.SemaphoreType.DMA
    return pl.pallas_call(
        expert_kernel,
        out_shape=(jax.ShapeDtypeStruct((PEERS, capacity, d_model), bf16),
                   jax.ShapeDtypeStruct((PEERS, 8, 256), f32),
                   jax.ShapeDtypeStruct((3, block, width), f32)),
        in_specs=[vmem, vmem, vmem, hbm],
        out_specs=[hbm, vmem, vmem],
        scratch_shapes=[
            pltpu.VMEM((2, 3, d_model, CHUNK), bf16),
            pltpu.VMEM((chunks, 3, d_model, CHUNK), f32),
            pltpu.VMEM((chunks, HALF, 3, block, CHUNK), f32),
            pltpu.VMEM((chunks, HALF - 1, 3, block, CHUNK), f32),
            pltpu.VMEM((n_rows, d_model), f32),
            pltpu.VMEM((PEERS, capacity, d_model), bf16),
            pltpu.VMEM((n_rows, 128), f32),
            pltpu.VMEM((PEERS, 8, 256), f32),
            dma((2,)), dma((2,)), dma((PEERS - 1, 2)), dma((PEERS - 1, 2)),
            dma((chunks, 2, 2)), dma((chunks, HALF, 2, 2)),
        ],
        compiler_params=pltpu.CompilerParams(
            collective_id=1, has_side_effects=True, vmem_limit_bytes=67043328),
        name="expert_step",
    )(x, dy, g, w)


def mm(a, b, dims):
    return lax.dot_general(a, b, (dims, ((), ())), preferred_element_type=jnp.float32)


def solution(mesh):
    tok_spec = P(("fsdp", "ep"), None)
    spec_in = P("ep", "fsdp", None)
    spec_out = P("ep", None, "fsdp")

    def per_device(x_tok, dy_tok, expert_ids, route_w, w_gate, w_up, w_down):
        tok_dev, top_k = expert_ids.shape
        d_model = x_tok.shape[1]
        d_ff = w_gate.shape[2]
        capacity = capacity_of(tok_dev, top_k, PEERS)
        me = lax.axis_index("ep")
        f32, bf16 = jnp.float32, jnp.bfloat16
        meta = jnp.concatenate([expert_ids.T.astype(f32), route_w.T, jnp.zeros((4, tok_dev), f32)], axis=0)
        w_local = jnp.stack([w_gate[0], w_up[0], w_down[0].T])
        x_all, dy_all, meta_all, w_all = gather_all(x_tok, dy_tok, meta, w_local)

        ids_all = meta_all[:, 0:top_k]
        hit = ids_all == me.astype(f32)
        mine = jnp.any(hit, axis=1)
        count = mine.astype(jnp.int32)
        place = jnp.where(mine, jnp.cumsum(count, axis=1) - count, capacity)
        pick = place[:, None, :] == jnp.arange(capacity, dtype=jnp.int32)[None, :, None]
        weight = jnp.sum(jnp.where(hit, meta_all[:, top_k:2 * top_k], 0.0), axis=1)
        gate_rows = jnp.sum(jnp.where(pick, weight[:, None, :], 0.0), axis=2).reshape(-1)
        pick = pick.astype(bf16)
        x_rows = jnp.einsum("sct,std->scd", pick, x_all, preferred_element_type=f32).astype(bf16)
        dy_rows = jnp.einsum("sct,std->scd", pick, dy_all, preferred_element_type=f32).astype(bf16)
        x_rows, dy_rows = x_rows.reshape(-1, d_model), dy_rows.reshape(-1, d_model)

        scaled_dy = (gate_rows[:, None] * dy_rows.astype(f32)).astype(bf16)
        dx_back, dr_back, g = expert_step(x_rows, dy_rows, scaled_dy, w_all.reshape(3, d_model, d_ff), capacity)

        onehot = expert_ids[:, :, None] == jnp.arange(PEERS, dtype=jnp.int32)
        used = jnp.any(onehot, axis=1).astype(jnp.int32)
        before = jnp.cumsum(used, axis=0) - used
        spot = jnp.sum(jnp.where(onehot, before[:, None, :], 0), axis=2)
        n_slots = PEERS * capacity
        slot = jnp.where(spot < capacity, expert_ids * capacity + spot, n_slots)
        at = slot[:, :, None] == jnp.arange(n_slots, dtype=jnp.int32)
        dr_flat = dr_back[:, 0, :capacity].reshape(-1)
        route_grad = jnp.sum(jnp.where(at, dr_flat, 0.0), axis=2)
        grad_x = mm(jnp.any(at, axis=1).astype(bf16), dx_back.reshape(n_slots, d_model), ((1,), (0,))).astype(bf16)
        return grad_x, route_grad, g[0][None], g[1][None], g[2].T[None]

    return jax.shard_map(
        per_device, mesh=mesh,
        in_specs=(tok_spec, tok_spec, tok_spec, tok_spec, spec_in, spec_in, spec_out),
        out_specs=(tok_spec, tok_spec, spec_in, spec_in, spec_out),
        check_vma=False)
```

```python
import jax
import jax.numpy as jnp
from jax import lax
from jax.experimental import pallas as pl
from jax.experimental.pallas import tpu as pltpu
from jax.sharding import PartitionSpec as P

CAP_FACTOR = 3
MESH = pl.DeviceIdType.MESH
NZ, NY, NX = 8, 4, 4
RING = NZ * NY
HALF = RING // 2
PEERS = 8


def capacity_of(tok_dev, top_k, experts):
    return max(8, ((CAP_FACTOR * tok_dev * top_k // experts + 7) // 8) * 8)


def ring_pos(k, i):
    z, y = lax.div(i, NY), lax.rem(i, NY)
    if k == 0:
        return z * NY + lax.rem(y + z, NY)
    o = lax.rem(z - 3 * y + 16, NZ)
    return NY * y + lax.rem(o, NY) + HALF * lax.div(o, NY)


def ring_dev(k, p):
    p = lax.rem(p + 2 * RING, RING)
    a, b = lax.div(p, NY), lax.rem(p, NY)
    if k == 0:
        z, y = a, lax.rem(b - a + 8, NY)
    else:
        z, y = lax.rem(3 * a + b, NZ), lax.rem(a, NY)
    return z * NY + y


def signal_all(targets):
    barrier = pltpu.get_barrier_semaphore()
    for t in targets:
        pl.semaphore_signal(barrier, inc=1, device_id=t, device_id_type=MESH)
    pl.semaphore_wait(barrier, len(targets))


def gather_kernel(x_ref, dy_ref, meta_ref, w_ref, xall, dyall, metaall, wall,
                  loc_sem, wsend, wrecv, tsend, trecv):
    i, p = lax.axis_index("fsdp"), lax.axis_index("ep")
    chip, core = lax.div(p, 2), lax.rem(p, 2)
    xr = lax.rem(chip + 1, NX) * 2 + core
    xl = lax.rem(chip + NX - 1, NX) * 2 + core
    xo = lax.rem(chip + 2, NX) * 2 + core
    partner = chip * 2 + 1 - core
    pos = [ring_pos(k, i) for k in (0, 1)]
    hop = [[ring_dev(k, pos[k] + 1), ring_dev(k, pos[k] - 1)] for k in (0, 1)]
    signal_all([{"fsdp": hop[k][d]} for k in (0, 1) for d in (0, 1)] + [{"ep": e} for e in (xr, xl, partner)])

    width = w_ref.shape[-1]
    nsub = wsend.shape[2]
    cols = width // (2 * nsub)

    own = [pltpu.make_async_copy(s, d, loc_sem.at[n]) for n, (s, d) in enumerate(
        ((x_ref, xall.at[p]), (dy_ref, dyall.at[p]), (meta_ref, metaall.at[p]), (w_ref, wall.at[:, i])))]
    for c in own:
        c.start()

    def wcopy(s, k, d, u, src=None):
        t = ring_dev(k, pos[k] - s if d == 0 else pos[k] + s)
        sl = pl.ds(k * (width // 2) + u * cols, cols)
        dst = wall.at[:, t, :, sl]
        return pltpu.make_async_remote_copy(
            src_ref=w_ref.at[:, :, sl] if src is None else dst, dst_ref=dst,
            send_sem=wsend.at[k, d, u], recv_sem=wrecv.at[s, k, d, u],
            device_id={"fsdp": hop[k][d]}, device_id_type=MESH)

    def tcopy(n, which, block, to, own_block=False):
        src, dst = ((x_ref, xall), (dy_ref, dyall), (meta_ref, metaall))[which]
        return pltpu.make_async_remote_copy(
            src_ref=src if own_block else dst.at[block], dst_ref=dst.at[block],
            send_sem=tsend.at[n], recv_sem=trecv.at[n],
            device_id={"ep": to}, device_id_type=MESH)

    subs = [(k, d, u) for u in range(nsub) for k in (0, 1) for d in (0, 1)]
    for k, d, u in subs:
        wcopy(0, k, d, u).start()
    first = [tcopy(3 * r + w, w, p, to, True) for r, to in ((0, xr), (1, xl), (2, partner)) for w in (2, 0, 1)]
    for c in first:
        c.start()

    def step(s):
        for k, d, u in subs:
            wcopy(s - 1, k, d, u, 1).wait_recv()
            wcopy(s - 1, k, d, u, 1).wait_send()
            wcopy(s, k, d, u, 1).start()

    def run(lo, hi):
        def body(s, c):
            step(s)
            return c
        lax.fori_loop(lo, hi, body, 0)

    run(1, 6)
    second, fwd = [], []
    for r, src in ((0, xl), (1, xr)):
        for w in (2, 0, 1):
            tcopy(3 * r + w, w, src, xr).wait_recv()
    for n, w, src, to in ((18 + 2, 2, xl, xr), (18 + 1, 1, xl, xr), (18 + 0, 0, xr, xl)):
        second.append(tcopy(n, w, src, to))
        second[-1].start()
    for r, src in ((3, xl), (4, xr)):
        for w in (2, 0, 1):
            fwd.append(tcopy(3 * r + w, w, src, partner))
            fwd[-1].start()
    run(6, 11)
    for n, w in ((18 + 2, 2), (18 + 1, 1), (18 + 0, 0)):
        tcopy(n, w, xo, xr).wait_recv()
    for w in (2, 0, 1):
        fwd.append(tcopy(15 + w, w, xo, partner))
        fwd[-1].start()
    run(11, HALF - 1)
    for k, d, u in subs:
        wcopy(HALF - 2, k, d, u, 1).wait_recv()
        wcopy(HALF - 2, k, d, u, 1).wait_send()
        if d == 0:
            wcopy(HALF - 1, k, d, u, 1).start()
    for c in first + second + fwd:
        c.wait_send()
    xpr, xpl = lax.rem(chip + 1, NX) * 2 + 1 - core, lax.rem(chip + NX - 1, NX) * 2 + 1 - core
    xpo = lax.rem(chip + 2, NX) * 2 + 1 - core
    for r, src in ((2, partner), (3, xpl), (4, xpr), (5, xpo)):
        for w in (2, 0, 1):
            tcopy(3 * r + w, w, src, partner).wait_recv()
    for c in own:
        c.wait()
    for k, d, u in subs:
        if d == 0:
            wcopy(HALF - 1, k, d, u, 1).wait_recv()
            wcopy(HALF - 1, k, d, u, 1).wait_send()


def gather_all(x_tok, dy_tok, meta, w):
    nsub = 4
    n3, rows, width = w.shape
    return pl.pallas_call(
        gather_kernel,
        out_shape=(jax.ShapeDtypeStruct((PEERS, *x_tok.shape), x_tok.dtype),
                   jax.ShapeDtypeStruct((PEERS, *dy_tok.shape), dy_tok.dtype),
                   jax.ShapeDtypeStruct((PEERS, *meta.shape), meta.dtype),
                   jax.ShapeDtypeStruct((n3, RING, rows, width), w.dtype)),
        in_specs=[pl.BlockSpec(memory_space=pltpu.VMEM)] * 4,
        out_specs=[pl.BlockSpec(memory_space=pltpu.VMEM)] * 4,
        scratch_shapes=[
            pltpu.SemaphoreType.DMA((4,)),
            pltpu.SemaphoreType.DMA((2, 2, nsub)),
            pltpu.SemaphoreType.DMA((HALF, 2, 2, nsub)),
            pltpu.SemaphoreType.DMA((21,)),
            pltpu.SemaphoreType.DMA((21,)),
        ],
        compiler_params=pltpu.CompilerParams(
            collective_id=0, has_side_effects=True, vmem_limit_bytes=60000 * 1024),
        name="gather_all",
    )(x_tok, dy_tok, meta, w)


CHUNK = 256
ROWS = 512
SUB = 256
HOPS = 6
SERVE = (1, 3)


def dot(a, b, ca, cb):
    return lax.dot_general(a, b, (((ca,), (cb,)), ((), ())), preferred_element_type=jnp.float32)


def expert_kernel(x_ref, dy_ref, g_ref, w_hbm, dx_out, dr_out, g_out,
                  wbuf, dw, az_half, az, ay_part, ay, by_half, by, bz_part, bz,
                  xt, gt, hid, dx_acc, dx_send, dr_acc, dr_send,
                  w_sem, loc_sem, xsend, xrecv, gsend, grecv):
    f32, bf16 = jnp.float32, jnp.bfloat16
    i, p = lax.axis_index("fsdp"), lax.axis_index("ep")
    z, y = lax.div(i, NY), lax.rem(i, NY)
    step_of = (1, -1)

    def zt(d, j):
        return lax.rem(z + step_of[d] * j + NZ, NZ)

    def yt(d, j):
        return lax.rem(y + step_of[d] * j + NY, NY)

    fz = [zt(d, 1) * NY + y for d in (0, 1)]
    fy = [z * NY + yt(d, 1) for d in (0, 1)]
    peer = [lax.rem(p + r, PEERS) for r in range(1, PEERS)]
    signal_all([{"fsdp": t} for t in fz + fy] + [{"ep": e} for e in peer])

    chunks = dw.shape[0]
    tiles = x_ref.shape[0] // ROWS
    half = CHUNK // 2
    ca, cb = pl.ds(0, half), pl.ds(half, half)
    part = (pl.ds(0, 16), pl.ds(16, 8))

    def wload(c):
        return pltpu.make_async_copy(
            w_hbm.at[:, :, pl.ds(pl.multiple_of(c * CHUNK, CHUNK), CHUNK)], wbuf.at[lax.rem(c, 2)],
            w_sem.at[lax.rem(c, 2)])

    def hop_a(c, h, d):
        if h == 0:
            return dw.at[c, :, zt(d, 4), pl.ds(2 * d, 2), :, ca], az_half.at[c, d], fz[d]
        if h < 4:
            return dw.at[c, :, zt(d, 4 - h), :, :, ca], az.at[c, d, h - 1], fz[d]
        if h == 4:
            return dw.at[c, :, z, yt(d, 2), part[d], ca], ay_part.at[c, d, :, pl.ds(0, part[d].size)], fy[d]
        return dw.at[c, :, z, yt(d, 1), :, ca], ay.at[c, d], fy[d]

    def land_a(c, h, d):
        if h == 0:
            return dw.at[c, :, zt(d, 3), pl.ds(2 * d, 2), :, ca]
        if h < 4:
            return dw.at[c, :, zt(d, 3 - h), :, :, ca]
        if h == 4:
            return dw.at[c, :, z, yt(d, 1), part[d], ca]
        return dw.at[c, :, z, y, :, ca]

    def hop_b(c, h, d):
        if h == 0:
            return dw.at[c, :, pl.ds(4 * d, 4), yt(d, 2), :, cb], by_half.at[c, d], fy[d]
        if h == 1:
            return dw.at[c, :, :, yt(d, 1), :, cb], by.at[c, d], fy[d]
        if h == 2:
            return dw.at[c, :, zt(d, 4), y, part[d], cb], bz_part.at[c, d, :, pl.ds(0, part[d].size)], fz[d]
        return dw.at[c, :, zt(d, 6 - h), y, :, cb], bz.at[c, d, h - 3], fz[d]

    def land_b(c, h, d):
        if h == 0:
            return dw.at[c, :, pl.ds(4 * d, 4), yt(d, 1), :, cb]
        if h == 1:
            return dw.at[c, :, :, y, :, cb]
        if h == 2:
            return dw.at[c, :, zt(d, 3), y, part[d], cb]
        return dw.at[c, :, zt(d, 5 - h), y, :, cb]

    rounds = len(SERVE)
    plans = ((hop_a, land_a), (hop_b, land_b))
    last_of_phase = ((3, 5), (1, 5))

    def gcopy(c, h, v, d):
        src, dst, to = plans[v][0](c, h, d)
        return pltpu.make_async_remote_copy(
            src_ref=src, dst_ref=dst, send_sem=gsend.at[c, v, d], recv_sem=grecv.at[c, h, v, d],
            device_id={"fsdp": to}, device_id_type=MESH)

    def arrive(c, h, v, d):
        gcopy(c, h, v, d).wait_recv()
        gcopy(c, h, v, d).wait_send()
        into, slot = plans[v][1](c, h, d), plans[v][0](c, h, d)[1]
        into[...] = into[...] + slot[...]

    def serve(q):
        lo = lax.max(lax.div(q - HOPS + rounds - 1 + rounds * chunks, rounds) - chunks - 1, 0)
        hi = lax.min(lax.div(q, rounds), chunks)

        def one(c, carry):
            s = q - (c + 1) * rounds
            for h in range(HOPS + 1):
                @pl.when(s == h)
                def _(h=h):
                    for v in (0, 1):
                        together = h - 1 in last_of_phase[v]
                        if together:
                            for d in (0, 1):
                                arrive(c, h - 1, v, d)
                        for d in (0, 1):
                            if h and not together:
                                arrive(c, h - 1, v, d)
                            if h < HOPS:
                                gcopy(c, h, v, d).start()
                    if h == HOPS:
                        out = pl.ds(pl.multiple_of(c * CHUNK, CHUNK), CHUNK)
                        g_out[:, :, out] = dw[c, :, z, y]
            return carry
        lax.fori_loop(lo, hi, one, 0)

    def forward(c, r):
        w = wbuf.at[lax.rem(c, 2)]
        for m in range(r * ROWS, (r + 1) * ROWS, SUB):
            rows = pl.ds(m, SUB)
            h1, h3 = dot(x_ref[rows, :], w[0], 1, 0), dot(x_ref[rows, :], w[1], 1, 0)
            da, u = dot(g_ref[rows, :], w[2], 1, 0), dot(dy_ref[rows, :], w[2], 1, 0)
            s = jax.nn.sigmoid(h1)
            a = (h1 * s * h3).astype(bf16)
            hid[0, rows, :] = (da * h3 * s * (1.0 + h1 * (1.0 - s))).astype(bf16)
            hid[1, rows, :] = (da * h1 * s).astype(bf16)
            hid[2, rows, :] = a
            au = a.astype(f32) * u
            dr_acc[rows, :] += au[:, :128] + au[:, 128:]

    def back(c, r):
        w = wbuf.at[lax.rem(c, 2)]
        for m in range(r * ROWS, (r + 1) * ROWS, SUB):
            rows = pl.ds(m, SUB)
            dx_acc[rows, :] += dot(hid[0, rows, :], w[0], 1, 1) + dot(hid[1, rows, :], w[1], 1, 1)

    def weight_grads(c):
        for n, t in enumerate((xt, xt, gt)):
            dw[c, n] = dot(t[...], hid[n], 1, 0).reshape(dw.shape[2:])

    wload(0).start()
    xt[...] = jnp.transpose(x_ref[...])
    gt[...] = jnp.transpose(g_ref[...])
    dr_acc[...] = jnp.zeros_like(dr_acc)
    dx_acc[...] = jnp.zeros_like(dx_acc)

    def step(c, carry):
        wload(c).wait()

        @pl.when(c + 1 < chunks)
        def _():
            wload(c + 1).start()
        for r in range(tiles + 1):
            if r < tiles:
                forward(c, r)
            else:
                weight_grads(c)
            if r:
                back(c, r - 1)
            if r in SERVE:
                serve(c * rounds + SERVE.index(r) + 1)
        return carry
    lax.fori_loop(0, chunks, step, 0)

    dx_send[...] = dx_acc[...].astype(bf16).reshape(dx_send.shape)
    total = jnp.sum(jnp.transpose(dr_acc[...]), axis=0, keepdims=True)
    cap = dx_send.shape[1]
    for e in range(PEERS):
        dr_send[e, 0:1, 0:cap] = total[:, e * cap:(e + 1) * cap]

    pairs = ((dx_send, dx_out), (dr_send, dr_out))
    own = [pltpu.make_async_copy(s.at[p], d.at[p], loc_sem.at[n]) for n, (s, d) in enumerate(pairs)]

    def xcopy(r, which, dst_peer, slot):
        src, dst = pairs[which]
        return pltpu.make_async_remote_copy(
            src_ref=src.at[dst_peer], dst_ref=dst.at[slot],
            send_sem=xsend.at[r, which], recv_sem=xrecv.at[r, which],
            device_id={"ep": dst_peer}, device_id_type=MESH)

    sent = [xcopy(r, w, peer[r], p) for r in range(PEERS - 1) for w in (0, 1)]
    for c in own + sent:
        c.start()

    def tail(q, carry):
        serve(q)
        return carry
    lax.fori_loop(rounds * chunks + 1, rounds * chunks + HOPS + 1, tail, 0)

    for c in sent:
        c.wait_send()
    for r in range(PEERS - 1):
        for w in (0, 1):
            xcopy(r, w, peer[r], lax.rem(p + PEERS - 1 - r, PEERS)).wait_recv()
    for c in own:
        c.wait()


def expert_step(x, dy, g, w, capacity):
    n_rows, d_model = x.shape
    width = w.shape[2]
    block, chunks, half = d_model // RING, width // CHUNK, CHUNK // 2
    f32, bf16 = jnp.float32, jnp.bfloat16
    vmem = pl.BlockSpec(memory_space=pltpu.VMEM)
    hbm = pl.BlockSpec(memory_space=pl.ANY)
    dma = pltpu.SemaphoreType.DMA
    return pl.pallas_call(
        expert_kernel,
        out_shape=(jax.ShapeDtypeStruct((PEERS, capacity, d_model), bf16),
                   jax.ShapeDtypeStruct((PEERS, 8, 256), f32),
                   jax.ShapeDtypeStruct((3, block, width), f32)),
        in_specs=[vmem, vmem, vmem, hbm],
        out_specs=[hbm, vmem, vmem],
        scratch_shapes=[
            pltpu.VMEM((2, 3, d_model, CHUNK), bf16),
            pltpu.VMEM((chunks, 3, NZ, NY, block, CHUNK), f32),
            pltpu.VMEM((chunks, 2, 3, NY // 2, block, half), f32),
            pltpu.VMEM((chunks, 2, 3, 3, NY, block, half), f32),
            pltpu.VMEM((chunks, 2, 3, 16, half), f32),
            pltpu.VMEM((chunks, 2, 3, block, half), f32),
            pltpu.VMEM((chunks, 2, 3, NZ // 2, block, half), f32),
            pltpu.VMEM((chunks, 2, 3, NZ, block, half), f32),
            pltpu.VMEM((chunks, 2, 3, 16, half), f32),
            pltpu.VMEM((chunks, 2, 3, 3, block, half), f32),
            pltpu.VMEM((d_model, n_rows), bf16),
            pltpu.VMEM((d_model, n_rows), bf16),
            pltpu.VMEM((3, n_rows, CHUNK), bf16),
            pltpu.VMEM((n_rows, d_model), f32),
            pltpu.VMEM((PEERS, capacity, d_model), bf16),
            pltpu.VMEM((n_rows, 128), f32),
            pltpu.VMEM((PEERS, 8, 256), f32),
            dma((2,)), dma((2,)), dma((PEERS - 1, 2)), dma((PEERS - 1, 2)),
            dma((chunks, 2, 2)), dma((chunks, HOPS, 2, 2)),
        ],
        compiler_params=pltpu.CompilerParams(
            collective_id=1, has_side_effects=True, vmem_limit_bytes=67043328),
        name="expert_step",
    )(x, dy, g, w)


def mm(a, b, dims):
    return lax.dot_general(a, b, (dims, ((), ())), preferred_element_type=jnp.float32)


def solution(mesh):
    tok_spec = P(("fsdp", "ep"), None)
    spec_in = P("ep", "fsdp", None)
    spec_out = P("ep", None, "fsdp")

    def per_device(x_tok, dy_tok, expert_ids, route_w, w_gate, w_up, w_down):
        tok_dev, top_k = expert_ids.shape
        d_model = x_tok.shape[1]
        d_ff = w_gate.shape[2]
        capacity = capacity_of(tok_dev, top_k, PEERS)
        me = lax.axis_index("ep")
        f32, bf16 = jnp.float32, jnp.bfloat16
        meta = jnp.concatenate([expert_ids.T.astype(f32), route_w.T, jnp.zeros((4, tok_dev), f32)], axis=0)
        w_local = jnp.stack([w_gate[0], w_up[0], w_down[0].T])
        x_all, dy_all, meta_all, w_all = gather_all(x_tok, dy_tok, meta, w_local)

        ids_all = meta_all[:, 0:top_k]
        hit = ids_all == me.astype(f32)
        mine = jnp.any(hit, axis=1)
        count = mine.astype(jnp.int32)
        place = jnp.where(mine, jnp.cumsum(count, axis=1) - count, capacity)
        pick = place[:, None, :] == jnp.arange(capacity, dtype=jnp.int32)[None, :, None]
        weight = jnp.sum(jnp.where(hit, meta_all[:, top_k:2 * top_k], 0.0), axis=1)
        gate_rows = jnp.sum(jnp.where(pick, weight[:, None, :], 0.0), axis=2).reshape(-1)
        pick = pick.astype(bf16)
        x_rows = jnp.einsum("sct,std->scd", pick, x_all, preferred_element_type=f32).astype(bf16)
        dy_rows = jnp.einsum("sct,std->scd", pick, dy_all, preferred_element_type=f32).astype(bf16)
        x_rows, dy_rows = x_rows.reshape(-1, d_model), dy_rows.reshape(-1, d_model)

        scaled_dy = (gate_rows[:, None] * dy_rows.astype(f32)).astype(bf16)
        dx_back, dr_back, g = expert_step(x_rows, dy_rows, scaled_dy, w_all.reshape(3, d_model, d_ff), capacity)

        onehot = expert_ids[:, :, None] == jnp.arange(PEERS, dtype=jnp.int32)
        used = jnp.any(onehot, axis=1).astype(jnp.int32)
        before = jnp.cumsum(used, axis=0) - used
        spot = jnp.sum(jnp.where(onehot, before[:, None, :], 0), axis=2)
        n_slots = PEERS * capacity
        slot = jnp.where(spot < capacity, expert_ids * capacity + spot, n_slots)
        at = slot[:, :, None] == jnp.arange(n_slots, dtype=jnp.int32)
        dr_flat = dr_back[:, 0, :capacity].reshape(-1)
        route_grad = jnp.sum(jnp.where(at, dr_flat, 0.0), axis=2)
        grad_x = mm(jnp.any(at, axis=1).astype(bf16), dx_back.reshape(n_slots, d_model), ((1,), (0,))).astype(bf16)
        return grad_x, route_grad, g[0][None], g[1][None], g[2].T[None]

    return jax.shard_map(
        per_device, mesh=mesh,
        in_specs=(tok_spec, tok_spec, tok_spec, tok_spec, spec_in, spec_in, spec_out),
        out_specs=(tok_spec, tok_spec, spec_in, spec_in, spec_out),
        check_vma=False)
```

```python
import jax
import jax.numpy as jnp
from jax import lax
from jax.experimental import pallas as pl
from jax.experimental.pallas import tpu as pltpu
from jax.sharding import PartitionSpec as P

CAP_FACTOR = 3
MESH = pl.DeviceIdType.MESH
NZ, NY, NX = 8, 4, 4
RING = NZ * NY
PEERS = 8


def capacity_of(tok_dev, top_k, experts):
    return max(8, ((CAP_FACTOR * tok_dev * top_k // experts + 7) // 8) * 8)


def signal_all(targets):
    barrier = pltpu.get_barrier_semaphore()
    for t in targets:
        pl.semaphore_signal(barrier, inc=1, device_id=t, device_id_type=MESH)
    pl.semaphore_wait(barrier, len(targets))


CHUNK = 256
ROWS = 512
SUB = 256
HOPS = 6
SERVE = (1, 3)
SETS = 4


def dot(a, b, ca, cb):
    return lax.dot_general(a, b, (((ca,), (cb,)), ((), ())), preferred_element_type=jnp.float32)


def moe_kernel(x_hbm, dy_hbm, ids_ref, r_ref, w1_ref, w3_ref, w2_ref, gx_out, rw_out, g1_out, g3_out, g2_out, x_all, dy_all,
               meta_ref, meta_all, dx_in, dr_in, tok, wbuf, dw, az_half, az, ay_part, ay, by_half, by, bz_part, bz,
               xs, dys, gs, xt, gt, hid, dx_acc, dr_acc, dr_send,
               tok_sem, loc_sem, tsend, trecv, wsend, wrecv, xsend, xrecv, gsend, grecv, free_sem):
    f32, bf16 = jnp.float32, jnp.bfloat16
    i, p = lax.axis_index("fsdp"), lax.axis_index("ep")
    z, y = lax.div(i, NY), lax.rem(i, NY)
    chip, core = lax.div(p, 2), lax.rem(p, 2)
    right, left, across = [lax.rem(chip + n, NX) for n in (1, NX - 1, 2)]
    xr, xl, xo = [n * 2 + core for n in (right, left, across)]
    partner, xpr, xpl, xpo = [n * 2 + 1 - core for n in (chip, right, left, across)]
    step_of = (1, -1)

    def zt(d, j):
        return lax.rem(z + step_of[d] * j + NZ, NZ)

    def yt(d, j):
        return lax.rem(y + step_of[d] * j + NY, NY)

    fz = [zt(d, 1) * NY + y for d in (0, 1)]
    fy = [z * NY + yt(d, 1) for d in (0, 1)]
    peer = [lax.rem(p + r, PEERS) for r in range(1, PEERS)]
    chunks = dw.shape[0]
    tiles = xs.shape[0] // ROWS
    cap = xs.shape[0] // PEERS
    half = CHUNK // 2
    ca, cb = pl.ds(0, half), pl.ds(half, half)

    tokens = ids_ref.shape[1]
    expert = lax.broadcasted_iota(jnp.int32, (PEERS, tokens), 0)
    hits = [expert == ids_ref[j:j + 1, :] for j in (0, 1)]
    used = jnp.logical_or(hits[0], hits[1])
    earlier = (lax.broadcasted_iota(jnp.int32, (tokens, tokens), 0)
               < lax.broadcasted_iota(jnp.int32, (tokens, tokens), 1))
    before = dot(jnp.where(used, 1.0, 0.0).astype(bf16), jnp.where(earlier, 1.0, 0.0).astype(bf16), 1, 0)
    meta_ref[0:PEERS, :] = jnp.where(used, before, float(cap))
    meta_ref[PEERS:2 * PEERS, :] = sum(jnp.where(hits[j], r_ref[j:j + 1, :], 0.0) for j in (0, 1))
    meta_all[p] = meta_ref[...]

    signal_all([{"fsdp": t} for t in fz + fy] + [{"ep": e} for e in peer])
    part = (pl.ds(0, 16), pl.ds(16, 8))

    def whop(c, h, v, d):
        cols = (ca, cb)[v]
        if h == 0:
            return wbuf.at[c, :, z, y, :, cols], (fy, fz)[v][d]
        if v == 0:
            if h == 1:
                return wbuf.at[c, :, z, yt(d, -1), part[d], cols], fy[d]
            if h < 5:
                return wbuf.at[c, :, zt(d, 2 - h), :, :, cols], fz[d]
            return wbuf.at[c, :, zt(d, -3), pl.ds(2 * d, 2), :, cols], fz[d]
        if h < 3:
            return wbuf.at[c, :, zt(d, -h), y, :, cols], fz[d]
        if h == 3:
            return wbuf.at[c, :, zt(d, -3), y, part[d], cols], fz[d]
        if h == 4:
            return wbuf.at[c, :, :, y, :, cols], fy[d]
        return wbuf.at[c, :, pl.ds(4 * d, 4), yt(d, -1), :, cols], fy[d]

    def wcopy(c, h, v, d):
        block, to = whop(c, h, v, d)
        return pltpu.make_async_remote_copy(
            src_ref=block, dst_ref=block, send_sem=wsend.at[c, v, d], recv_sem=wrecv.at[c, h, v, d],
            device_id={"fsdp": to}, device_id_type=MESH)

    def gather_round(a):
        def one(c, carry):
            for h in range(HOPS + 1):
                @pl.when(a - c == h)
                def _(h=h):
                    for v in (0, 1):
                        together = h == (2, 4)[v]
                        for d in (0, 1):
                            if h:
                                wcopy(c, h - 1, v, d).wait_recv()
                                wcopy(c, h - 1, v, d).wait_send()
                            if h < HOPS and not together:
                                wcopy(c, h, v, d).start()
                        if together:
                            for d in (0, 1):
                                wcopy(c, h, v, d).start()
            return carry
        lax.fori_loop(lax.max(a - HOPS, 0), lax.min(a + 1, chunks), one, 0)

    def tcopy(n, which, block, to, own_block=False):
        src, dst = ((x_hbm, x_all), (dy_hbm, dy_all), (meta_ref, meta_all))[which]
        return pltpu.make_async_remote_copy(
            src_ref=src if own_block else dst.at[block], dst_ref=dst.at[block],
            send_sem=tsend.at[n], recv_sem=trecv.at[n],
            device_id={"ep": to}, device_id_type=MESH)

    def arrived(r, block):
        for w in (2, 0, 1):
            tcopy(3 * r + w, w, block, partner).wait_recv()

    def fetch(slot, block=None):
        for w, (own, ref) in enumerate(((x_hbm, x_all), (dy_hbm, dy_all))):
            yield pltpu.make_async_copy(own if block is None else ref.at[block], tok.at[slot, w], tok_sem.at[slot, w])

    def picked(place):
        return lax.broadcasted_iota(jnp.int32, (cap, tokens), 0).astype(f32) == place

    def build(slot, copies, meta, src):
        for c in copies:
            c.wait()
        place, weight = meta[pl.ds(p, 1), :], meta[pl.ds(PEERS + p, 1), :]
        pick = picked(place)
        rows = pl.ds(pl.multiple_of(src * cap, cap), cap)
        onehot = jnp.where(pick, 1.0, 0.0).astype(bf16)
        xs[rows, :] = dot(onehot, tok[slot, 0], 1, 0).astype(bf16)
        dy = dot(onehot, tok[slot, 1], 1, 0).astype(bf16)
        dys[rows, :] = dy
        gate = jnp.sum(jnp.where(pick, weight, 0.0), axis=1, keepdims=True)
        gs[rows, :] = (gate * dy.astype(f32)).astype(bf16)

    def build_pair(k, first, second):
        loads = [list(fetch(slot, None if src is None else src)) for slot, src in enumerate((first, second))]
        for cs in loads:
            for c in cs:
                c.start()
        for slot, src in enumerate((first, second)):
            build(slot, loads[slot], meta_ref if src is None else meta_all.at[src], p if src is None else src)
        both = pl.ds(pl.multiple_of(k * 2 * cap, 2 * cap), 2 * cap)
        xt[:, both] = jnp.transpose(xs[both, :])
        gt[:, both] = jnp.transpose(gs[both, :])

    def hop_a(c, h, d):
        if h == 0:
            return dw.at[c, :, zt(d, 4), pl.ds(2 * d, 2), :, ca], az_half.at[lax.rem(c, SETS), d], fz[d]
        if h < 4:
            return dw.at[c, :, zt(d, 4 - h), :, :, ca], az.at[lax.rem(c, SETS), d, h - 1], fz[d]
        if h == 4:
            return dw.at[c, :, z, yt(d, 2), part[d], ca], ay_part.at[lax.rem(c, SETS), d, :, pl.ds(0, part[d].size)], fy[d]
        return dw.at[c, :, z, yt(d, 1), :, ca], ay.at[lax.rem(c, SETS), d], fy[d]

    def land_a(c, h, d):
        if h == 0:
            return dw.at[c, :, zt(d, 3), pl.ds(2 * d, 2), :, ca]
        if h < 4:
            return dw.at[c, :, zt(d, 3 - h), :, :, ca]
        if h == 4:
            return dw.at[c, :, z, yt(d, 1), part[d], ca]
        return dw.at[c, :, z, y, :, ca]

    def hop_b(c, h, d):
        if h == 0:
            return dw.at[c, :, pl.ds(4 * d, 4), yt(d, 2), :, cb], by_half.at[lax.rem(c, SETS), d], fy[d]
        if h == 1:
            return dw.at[c, :, :, yt(d, 1), :, cb], by.at[lax.rem(c, SETS), d], fy[d]
        if h == 2:
            return dw.at[c, :, zt(d, 4), y, part[d], cb], bz_part.at[lax.rem(c, SETS), d, :, pl.ds(0, part[d].size)], fz[d]
        return dw.at[c, :, zt(d, 6 - h), y, :, cb], bz.at[lax.rem(c, SETS), d, h - 3], fz[d]

    def land_b(c, h, d):
        if h == 0:
            return dw.at[c, :, pl.ds(4 * d, 4), yt(d, 1), :, cb]
        if h == 1:
            return dw.at[c, :, :, y, :, cb]
        if h == 2:
            return dw.at[c, :, zt(d, 3), y, part[d], cb]
        return dw.at[c, :, zt(d, 5 - h), y, :, cb]

    rounds = len(SERVE)
    plans = ((hop_a, land_a), (hop_b, land_b))
    last_of_phase = ((3, 5), (1, 5))

    def gcopy(c, h, v, d):
        src, dst, to = plans[v][0](c, h, d)
        return pltpu.make_async_remote_copy(
            src_ref=src, dst_ref=dst, send_sem=gsend.at[c, v, d], recv_sem=grecv.at[c, h, v, d],
            device_id={"fsdp": to}, device_id_type=MESH)

    def arrive(c, h, v, d):
        gcopy(c, h, v, d).wait_recv()
        gcopy(c, h, v, d).wait_send()
        into, slot = plans[v][1](c, h, d), plans[v][0](c, h, d)[1]
        into[...] = into[...] + slot[...]

    def serve(q):
        lo = lax.max(lax.div(q - HOPS + rounds - 1 + rounds * chunks, rounds) - chunks - 1, 0)
        hi = lax.min(lax.div(q, rounds), chunks)

        def one(c, carry):
            s = q - (c + 1) * rounds
            for h in range(HOPS + 1):
                @pl.when(s == h)
                def _(h=h):
                    if h == 0:
                        @pl.when(c >= SETS)
                        def _():
                            pl.semaphore_wait(free_sem.at[lax.max(c - SETS, 0)], 4)
                    for v in (0, 1):
                        together = h - 1 in last_of_phase[v]
                        if together:
                            for d in (0, 1):
                                arrive(c, h - 1, v, d)
                        for d in (0, 1):
                            if h and not together:
                                arrive(c, h - 1, v, d)
                            if h < HOPS:
                                gcopy(c, h, v, d).start()
                    if h == HOPS:
                        out = pl.ds(pl.multiple_of(c * CHUNK, CHUNK), CHUNK)
                        for n, g in enumerate((g1_out, g3_out, g2_out)):
                            g[:, out] = dw[c, n, z, y]

                        @pl.when(c + SETS < chunks)
                        def _():
                            for t in fz + fy:
                                pl.semaphore_signal(free_sem.at[lax.min(c, chunks - SETS - 1)], inc=1,
                                                    device_id={"fsdp": t}, device_id_type=MESH)
            return carry
        lax.fori_loop(lo, hi, one, 0)

    def forward(c, r):
        w = [wbuf[c, n].reshape(xs.shape[1], CHUNK) for n in range(3)]
        for m in range(r * ROWS, (r + 1) * ROWS, SUB):
            rows = pl.ds(m, SUB)
            h1, h3 = dot(xs[rows, :], w[0], 1, 0), dot(xs[rows, :], w[1], 1, 0)
            da, u = dot(gs[rows, :], w[2], 1, 0), dot(dys[rows, :], w[2], 1, 0)
            s = jax.nn.sigmoid(h1)
            a = (h1 * s * h3).astype(bf16)
            hid[0, rows, :] = (da * h3 * s * (1.0 + h1 * (1.0 - s))).astype(bf16)
            hid[1, rows, :] = (da * h1 * s).astype(bf16)
            hid[2, rows, :] = a
            au = a.astype(f32) * u
            dr_acc[rows, :] += au[:, :128] + au[:, 128:]

    def back(c, r):
        w = [wbuf[c, n].reshape(xs.shape[1], CHUNK) for n in range(3)]
        for m in range(r * ROWS, (r + 1) * ROWS, SUB):
            rows = pl.ds(m, SUB)
            dx_acc[rows, :] += dot(hid[0, rows, :], w[0], 1, 1) + dot(hid[1, rows, :], w[1], 1, 1)

    def weight_grads(c):
        for n, t in enumerate((xt, xt, gt)):
            dw[c, n] = dot(t[...], hid[n], 1, 0).reshape(dw.shape[2:])

    first_sends = [tcopy(3 * r + w, w, p, to, True) for r, to in ((0, xr), (1, xl), (2, partner)) for w in (2, 0, 1)]
    for c in first_sends:
        c.start()

    def own_piece(c, carry):
        for n, w in enumerate((w1_ref, w3_ref, w2_ref)):
            wbuf[c, n, z, y] = w[:, pl.ds(pl.multiple_of(c * CHUNK, CHUNK), CHUNK)]
        return carry
    lax.fori_loop(0, chunks, own_piece, 0)
    dr_acc[...] = jnp.zeros_like(dr_acc)
    dx_acc[...] = jnp.zeros_like(dx_acc)

    second = [tcopy(n, w, src, to) for n, w, src, to in
              ((18 + 2, 2, xl, xr), (18 + 1, 1, xl, xr), (18 + 0, 0, xr, xl))]
    forward_lr = [tcopy(3 * r + w, w, src, partner) for r, src in ((3, xl), (4, xr)) for w in (2, 0, 1)]
    forward_o = [tcopy(15 + w, w, xo, partner) for w in (2, 0, 1)]

    def back_block(which, q):
        return xs.at[pl.ds(pl.multiple_of(q * cap, cap), cap)] if which == 0 else dr_send.at[q]

    def xcopy(r, which, dst_peer, slot):
        return pltpu.make_async_remote_copy(
            src_ref=back_block(which, dst_peer), dst_ref=(dx_in, dr_in)[which].at[slot],
            send_sem=xsend.at[r, which], recv_sem=xrecv.at[r, which],
            device_id={"ep": dst_peer}, device_id_type=MESH)

    own = [pltpu.make_async_copy(back_block(n, p), d.at[p], loc_sem.at[n]) for n, d in enumerate((dx_in, dr_in))]
    sent = [[xcopy(r, w, peer[r], p) for r in range(PEERS - 1)] for w in (0, 1)]

    def tokens_1():
        arrived(2, partner)
        build_pair(chip, None, partner)

    def tokens_3():
        arrived(0, xl)
        arrived(1, xr)
        for c in second + forward_lr:
            c.start()

    def tokens_4():
        arrived(3, xpl)
        build_pair(left, xl, xpl)

    def tokens_5():
        arrived(4, xpr)
        build_pair(right, xr, xpr)
        arrived(6, xo)
        for c in forward_o:
            c.start()

    def tokens_6():
        arrived(5, xpo)
        build_pair(across, xo, xpo)

    def send_back():
        xs[...] = dx_acc[...].astype(bf16)
        for c in own[:1] + sent[0]:
            c.start()
        for e in range(PEERS):
            total = jnp.sum(dr_acc[e * cap:(e + 1) * cap, :], axis=1, keepdims=True)
            here = picked(meta_all[e, pl.ds(p, 1), :])
            dr_send[e, 0:1, :] = jnp.sum(jnp.where(here, total, 0.0), axis=0, keepdims=True)
        for c in own[1:] + sent[1]:
            c.start()

    def combine():
        for r in range(PEERS - 1):
            for w in (0, 1):
                xcopy(r, w, peer[r], lax.rem(p + PEERS - 1 - r, PEERS)).wait_recv()
        for c in own:
            c.wait()
        gx = jnp.zeros(gx_out.shape, f32)
        rw = [jnp.zeros((1, tokens), f32) for _ in (0, 1)]
        for e in range(PEERS):
            here = jnp.where(picked(meta_ref[e:e + 1, :]), 1.0, 0.0).astype(bf16)
            gx = gx + dot(here, dx_in[e], 0, 0)
            rw = [rw[j] + jnp.where(ids_ref[j:j + 1, :] == e, dr_in[e, 0:1, :], 0.0) for j in (0, 1)]
        gx_out[...] = gx.astype(bf16)
        for j in (0, 1):
            rw_out[j:j + 1, :] = rw[j]

    def compute(c, r):
        if r < tiles:
            forward(c, r)
        else:
            weight_grads(c)
        if r:
            back(c, r - 1)

    lead = HOPS + 1
    steps = lead + rounds * chunks

    def step(t, carry):
        n = t - lead
        c, r = lax.div(lax.max(n, 0), rounds), lax.rem(lax.max(n, 0), rounds)
        for j in range(rounds):
            @pl.when(jnp.logical_and(jnp.logical_and(n >= 0, t < steps), r == j))
            def _(j=j):
                for u in range(0 if j == 0 else SERVE[j - 1] + 1, SERVE[j] + 1):
                    compute(c, u)

        @pl.when(r == 0)
        def _():
            gather_round(lax.min(t, lead) + c)
        for at, event in ((1, tokens_1), (3, tokens_3), (4, tokens_4), (5, tokens_5), (6, tokens_6),
                          (steps, send_back), (steps + HOPS - 1, combine)):
            pl.when(t == at)(event)

        @pl.when(n >= 0)
        def _():
            serve(n + 1)
        return carry
    lax.fori_loop(0, steps + HOPS, step, 0)

    for c in first_sends + second + forward_lr + forward_o + sent[0] + sent[1]:
        c.wait_send()


def moe_step(x_tok, dy_tok, ids, route, w1, w3, w2t, capacity):
    tok_dev, d_model = x_tok.shape
    width = w1.shape[1]
    n_rows = PEERS * capacity
    block, chunks, half = d_model // RING, width // CHUNK, CHUNK // 2
    f32, bf16 = jnp.float32, jnp.bfloat16
    vmem = pl.BlockSpec(memory_space=pltpu.VMEM)
    hbm = pl.BlockSpec(memory_space=pl.ANY)
    dma = pltpu.SemaphoreType.DMA
    landing = jax.ShapeDtypeStruct((PEERS, tok_dev, d_model), bf16)
    grad = jax.ShapeDtypeStruct((block, width), f32)
    meta = jax.ShapeDtypeStruct((2 * PEERS, tok_dev), f32)
    return pl.pallas_call(
        moe_kernel,
        out_shape=(jax.ShapeDtypeStruct((tok_dev, d_model), bf16), jax.ShapeDtypeStruct(route.shape, f32),
                   grad, grad, grad, landing, landing),
        in_specs=[hbm, hbm] + [vmem] * 5,
        out_specs=[vmem] * 5 + [hbm, hbm],
        scratch_shapes=[
            pltpu.VMEM(meta.shape, f32),
            pltpu.VMEM((PEERS, *meta.shape), f32),
            pltpu.VMEM((PEERS, capacity, d_model), bf16),
            pltpu.VMEM((PEERS, 8, tok_dev), f32),
            pltpu.VMEM((2, 2, tok_dev, d_model), bf16),
            pltpu.VMEM((chunks, 3, NZ, NY, block, CHUNK), bf16),
            pltpu.VMEM((chunks, 3, NZ, NY, block, CHUNK), f32),
            pltpu.VMEM((SETS, 2, 3, NY // 2, block, half), f32),
            pltpu.VMEM((SETS, 2, 3, 3, NY, block, half), f32),
            pltpu.VMEM((SETS, 2, 3, 16, half), f32),
            pltpu.VMEM((SETS, 2, 3, block, half), f32),
            pltpu.VMEM((SETS, 2, 3, NZ // 2, block, half), f32),
            pltpu.VMEM((SETS, 2, 3, NZ, block, half), f32),
            pltpu.VMEM((SETS, 2, 3, 16, half), f32),
            pltpu.VMEM((SETS, 2, 3, 3, block, half), f32),
            pltpu.VMEM((n_rows, d_model), bf16),
            pltpu.VMEM((n_rows, d_model), bf16),
            pltpu.VMEM((n_rows, d_model), bf16),
            pltpu.VMEM((d_model, n_rows), bf16),
            pltpu.VMEM((d_model, n_rows), bf16),
            pltpu.VMEM((3, n_rows, CHUNK), bf16),
            pltpu.VMEM((n_rows, d_model), f32),
            pltpu.VMEM((n_rows, 128), f32),
            pltpu.VMEM((PEERS, 8, tok_dev), f32),
            dma((2, 2)), dma((2,)), dma((21,)), dma((21,)),
            dma((chunks, 2, 2)), dma((chunks, HOPS, 2, 2)),
            dma((PEERS - 1, 2)), dma((PEERS - 1, 2)),
            dma((chunks, 2, 2)), dma((chunks, HOPS, 2, 2)),
            pltpu.SemaphoreType.REGULAR((chunks - SETS,)),
        ],
        compiler_params=pltpu.CompilerParams(
            collective_id=0, has_side_effects=True, vmem_limit_bytes=67043328),
        name="moe_step",
    )(x_tok, dy_tok, ids, route, w1, w3, w2t)


def solution(mesh):
    tok_spec = P(("fsdp", "ep"), None)
    spec_in = P("ep", "fsdp", None)
    spec_out = P("ep", None, "fsdp")

    def per_device(x_tok, dy_tok, expert_ids, route_w, w_gate, w_up, w_down):
        tok_dev, top_k = expert_ids.shape
        capacity = capacity_of(tok_dev, top_k, PEERS)
        gx, rw, g1, g3, g2, _, _ = moe_step(
            x_tok, dy_tok, expert_ids.T, route_w.T, w_gate[0], w_up[0], w_down[0].T, capacity)
        return gx, rw.T, g1[None], g3[None], g2.T[None]

    return jax.shard_map(
        per_device, mesh=mesh,
        in_specs=(tok_spec, tok_spec, tok_spec, tok_spec, spec_in, spec_in, spec_out),
        out_specs=(tok_spec, tok_spec, spec_in, spec_in, spec_out),
        check_vma=False)
```

```python
import jax
import jax.numpy as jnp
from jax import lax
from jax.experimental import pallas as pl
from jax.experimental.pallas import tpu as pltpu
from jax.sharding import PartitionSpec as P

CAP_FACTOR = 3
MESH = pl.DeviceIdType.MESH
NZ, NY, NX = 8, 4, 4
RING = NZ * NY
PEERS = 8


def capacity_of(tok_dev, top_k, experts):
    return max(8, ((CAP_FACTOR * tok_dev * top_k // experts + 7) // 8) * 8)


def signal_all(targets):
    barrier = pltpu.get_barrier_semaphore()
    for t in targets:
        pl.semaphore_signal(barrier, inc=1, device_id=t, device_id_type=MESH)
    pl.semaphore_wait(barrier, len(targets))


CHUNK = 256
ROWS = 512
SUB = 256
HOPS = 6
SERVE = (1, 3)
SETS = 4


def dot(a, b, ca, cb):
    return lax.dot_general(a, b, (((ca,), (cb,)), ((), ())), preferred_element_type=jnp.float32)


def moe_kernel(x_hbm, dy_hbm, ids_ref, r_ref, w1_ref, w3_ref, w2_ref, gx_out, rw_out, g_out, x_all, dy_all,
               meta_ref, meta_all, dx_in, dr_in, tok, wbuf, dw, az_half, az, ay_part, ay, by_half, by, bz_part, bz,
               xs, dys, gs, xt, gt, hid, dx_acc, dr_acc, dr_send,
               tok_sem, loc_sem, tsend, trecv, wsend, wrecv, xsend, xrecv, gsend, grecv, free_sem):
    f32, bf16 = jnp.float32, jnp.bfloat16
    i, p = lax.axis_index("fsdp"), lax.axis_index("ep")
    z, y = lax.div(i, NY), lax.rem(i, NY)
    chip, core = lax.div(p, 2), lax.rem(p, 2)
    right, left, across = [lax.rem(chip + n, NX) for n in (1, NX - 1, 2)]
    xr, xl, xo = [n * 2 + core for n in (right, left, across)]
    partner, xpr, xpl, xpo = [n * 2 + 1 - core for n in (chip, right, left, across)]
    step_of = (1, -1)

    def zt(d, j):
        return lax.rem(z + step_of[d] * j + NZ, NZ)

    def yt(d, j):
        return lax.rem(y + step_of[d] * j + NY, NY)

    fz = [zt(d, 1) * NY + y for d in (0, 1)]
    fy = [z * NY + yt(d, 1) for d in (0, 1)]
    peer = [lax.rem(p + r, PEERS) for r in range(1, PEERS)]
    chunks = dw.shape[0]
    tiles = xs.shape[0] // ROWS
    cap = xs.shape[0] // PEERS
    half = CHUNK // 2
    ca, cb = pl.ds(0, half), pl.ds(half, half)

    tokens = ids_ref.shape[1]
    expert = lax.broadcasted_iota(jnp.int32, (PEERS, tokens), 0)
    hits = [expert == ids_ref[j:j + 1, :] for j in (0, 1)]
    used = jnp.logical_or(hits[0], hits[1])
    earlier = (lax.broadcasted_iota(jnp.int32, (tokens, tokens), 0)
               < lax.broadcasted_iota(jnp.int32, (tokens, tokens), 1))
    before = dot(jnp.where(used, 1.0, 0.0).astype(bf16), jnp.where(earlier, 1.0, 0.0).astype(bf16), 1, 0)
    meta_ref[0:PEERS, :] = jnp.where(used, before, float(cap))
    meta_ref[PEERS:2 * PEERS, :] = sum(jnp.where(hits[j], r_ref[j:j + 1, :], 0.0) for j in (0, 1))
    meta_all[p] = meta_ref[...]

    signal_all([{"fsdp": t} for t in fz + fy] + [{"ep": e} for e in peer])
    part = (pl.ds(0, 16), pl.ds(16, 8))

    def whop(c, h, v, d):
        cols = (ca, cb)[v]
        if h == 0:
            return wbuf.at[c, :, z, y, :, cols], (fy, fz)[v][d]
        if v == 0:
            if h == 1:
                return wbuf.at[c, :, z, yt(d, -1), part[d], cols], fy[d]
            if h < 5:
                return wbuf.at[c, :, zt(d, 2 - h), :, :, cols], fz[d]
            return wbuf.at[c, :, zt(d, -3), pl.ds(2 * d, 2), :, cols], fz[d]
        if h < 3:
            return wbuf.at[c, :, zt(d, -h), y, :, cols], fz[d]
        if h == 3:
            return wbuf.at[c, :, zt(d, -3), y, part[d], cols], fz[d]
        if h == 4:
            return wbuf.at[c, :, :, y, :, cols], fy[d]
        return wbuf.at[c, :, pl.ds(4 * d, 4), yt(d, -1), :, cols], fy[d]

    def wcopy(c, h, v, d):
        block, to = whop(c, h, v, d)
        return pltpu.make_async_remote_copy(
            src_ref=block, dst_ref=block, send_sem=wsend.at[c, v, d], recv_sem=wrecv.at[c, h, v, d],
            device_id={"fsdp": to}, device_id_type=MESH)

    def gather_round(a):
        @pl.when(a < chunks)
        def _():
            for v in (0, 1):
                for d in (0, 1):
                    wcopy(lax.min(a, chunks - 1), 0, v, d).start()

        def one(c, carry):
            for h in range(1, HOPS + 1):
                @pl.when(a - c == h)
                def _(h=h):
                    for v in (0, 1):
                        together = h == (2, 4)[v]
                        for d in (0, 1):
                            wcopy(c, h - 1, v, d).wait_recv()
                            wcopy(c, h - 1, v, d).wait_send()
                            if h < HOPS and not together:
                                wcopy(c, h, v, d).start()
                        if together:
                            for d in (0, 1):
                                wcopy(c, h, v, d).start()
            return carry
        lax.fori_loop(lax.max(a - HOPS, 0), lax.min(a, chunks), one, 0)

    def tcopy(n, which, block, to, own_block=False):
        src, dst = ((x_hbm, x_all), (dy_hbm, dy_all), (meta_ref, meta_all))[which]
        return pltpu.make_async_remote_copy(
            src_ref=src if own_block else dst.at[block], dst_ref=dst.at[block],
            send_sem=tsend.at[n], recv_sem=trecv.at[n],
            device_id={"ep": to}, device_id_type=MESH)

    def arrived(r, block):
        for w in (2, 0, 1):
            tcopy(3 * r + w, w, block, partner).wait_recv()

    def fetch(slot, block=None):
        for w, (own, ref) in enumerate(((x_hbm, x_all), (dy_hbm, dy_all))):
            yield pltpu.make_async_copy(own if block is None else ref.at[block], tok.at[slot, w], tok_sem.at[slot, w])

    def picked(place):
        return lax.broadcasted_iota(jnp.int32, (cap, tokens), 0).astype(f32) == place

    def build(slot, copies, meta, src):
        for c in copies:
            c.wait()
        place, weight = meta[pl.ds(p, 1), :], meta[pl.ds(PEERS + p, 1), :]
        pick = picked(place)
        rows = pl.ds(pl.multiple_of(src * cap, cap), cap)
        onehot = jnp.where(pick, 1.0, 0.0).astype(bf16)
        xs[rows, :] = dot(onehot, tok[slot, 0], 1, 0).astype(bf16)
        dy = dot(onehot, tok[slot, 1], 1, 0).astype(bf16)
        dys[rows, :] = dy
        gate = jnp.sum(jnp.where(pick, weight, 0.0), axis=1, keepdims=True)
        gs[rows, :] = (gate * dy.astype(f32)).astype(bf16)

    def build_pair(k, first, second):
        loads = [list(fetch(slot, None if src is None else src)) for slot, src in enumerate((first, second))]
        for cs in loads:
            for c in cs:
                c.start()
        for slot, src in enumerate((first, second)):
            build(slot, loads[slot], meta_ref if src is None else meta_all.at[src], p if src is None else src)
        both = pl.ds(pl.multiple_of(k * 2 * cap, 2 * cap), 2 * cap)
        xt[:, both] = jnp.transpose(xs[both, :])
        gt[:, both] = jnp.transpose(gs[both, :])

    def hop_a(c, h, d):
        if h == 0:
            return dw.at[c, :, zt(d, 4), pl.ds(2 * d, 2), :, ca], az_half.at[lax.rem(c, SETS), d], fz[d]
        if h < 4:
            return dw.at[c, :, zt(d, 4 - h), :, :, ca], az.at[lax.rem(c, SETS), d, h - 1], fz[d]
        if h == 4:
            return dw.at[c, :, z, yt(d, 2), part[d], ca], ay_part.at[lax.rem(c, SETS), d, :, pl.ds(0, part[d].size)], fy[d]
        return dw.at[c, :, z, yt(d, 1), :, ca], ay.at[lax.rem(c, SETS), d], fy[d]

    def land_a(c, h, d):
        if h == 0:
            return dw.at[c, :, zt(d, 3), pl.ds(2 * d, 2), :, ca]
        if h < 4:
            return dw.at[c, :, zt(d, 3 - h), :, :, ca]
        if h == 4:
            return dw.at[c, :, z, yt(d, 1), part[d], ca]
        return dw.at[c, :, z, y, :, ca]

    def hop_b(c, h, d):
        if h == 0:
            return dw.at[c, :, pl.ds(4 * d, 4), yt(d, 2), :, cb], by_half.at[lax.rem(c, SETS), d], fy[d]
        if h == 1:
            return dw.at[c, :, :, yt(d, 1), :, cb], by.at[lax.rem(c, SETS), d], fy[d]
        if h == 2:
            return dw.at[c, :, zt(d, 4), y, part[d], cb], bz_part.at[lax.rem(c, SETS), d, :, pl.ds(0, part[d].size)], fz[d]
        return dw.at[c, :, zt(d, 6 - h), y, :, cb], bz.at[lax.rem(c, SETS), d, h - 3], fz[d]

    def land_b(c, h, d):
        if h == 0:
            return dw.at[c, :, pl.ds(4 * d, 4), yt(d, 1), :, cb]
        if h == 1:
            return dw.at[c, :, :, y, :, cb]
        if h == 2:
            return dw.at[c, :, zt(d, 3), y, part[d], cb]
        return dw.at[c, :, zt(d, 5 - h), y, :, cb]

    rounds = len(SERVE)
    plans = ((hop_a, land_a), (hop_b, land_b))
    last_of_phase = ((3, 5), (1, 5))

    def gcopy(c, h, v, d):
        src, dst, to = plans[v][0](c, h, d)
        return pltpu.make_async_remote_copy(
            src_ref=src, dst_ref=dst, send_sem=gsend.at[c, v, d], recv_sem=grecv.at[c, h, v, d],
            device_id={"fsdp": to}, device_id_type=MESH)

    def arrive(c, h, v, d):
        gcopy(c, h, v, d).wait_recv()
        gcopy(c, h, v, d).wait_send()
        into, slot = plans[v][1](c, h, d), plans[v][0](c, h, d)[1]
        into[...] = into[...] + slot[...]

    def serve(q):
        lo = lax.max(lax.div(q - HOPS + rounds - 1 + rounds * chunks, rounds) - chunks - 1, 0)
        hi = lax.min(lax.div(q, rounds), chunks)

        new = lax.div(q, rounds) - 1

        @pl.when(jnp.logical_and(lax.rem(q, rounds) == 0, jnp.logical_and(new >= 0, new < chunks)))
        def _():
            c = lax.min(lax.max(new, 0), chunks - 1)

            @pl.when(c >= SETS)
            def _():
                pl.semaphore_wait(free_sem.at[lax.max(c - SETS, 0)], 4)
            for v in (0, 1):
                for d in (0, 1):
                    gcopy(c, 0, v, d).start()

        def one(c, carry):
            s = q - (c + 1) * rounds
            for h in range(1, HOPS + 1):
                @pl.when(s == h)
                def _(h=h):
                    for v in (0, 1):
                        together = h - 1 in last_of_phase[v]
                        if together:
                            for d in (0, 1):
                                arrive(c, h - 1, v, d)
                        for d in (0, 1):
                            if h and not together:
                                arrive(c, h - 1, v, d)
                            if h < HOPS:
                                gcopy(c, h, v, d).start()
                    if h == HOPS:
                        out = pl.ds(pl.multiple_of(c * CHUNK, CHUNK), CHUNK)
                        g_out[:, :, out] = dw[c, :, z, y]

                        @pl.when(c + SETS < chunks)
                        def _():
                            for t in fz + fy:
                                pl.semaphore_signal(free_sem.at[lax.min(c, chunks - SETS - 1)], inc=1,
                                                    device_id={"fsdp": t}, device_id_type=MESH)
            return carry
        lax.fori_loop(lo, hi, one, 0)

    def forward(c, r):
        w = [wbuf[c, n].reshape(xs.shape[1], CHUNK) for n in range(3)]
        for m in range(r * ROWS, (r + 1) * ROWS, SUB):
            rows = pl.ds(m, SUB)
            h1, h3 = dot(xs[rows, :], w[0], 1, 0), dot(xs[rows, :], w[1], 1, 0)
            da, u = dot(gs[rows, :], w[2], 1, 0), dot(dys[rows, :], w[2], 1, 0)
            s = jax.nn.sigmoid(h1)
            a = (h1 * s * h3).astype(bf16)
            hid[0, rows, :] = (da * h3 * s * (1.0 + h1 * (1.0 - s))).astype(bf16)
            hid[1, rows, :] = (da * h1 * s).astype(bf16)
            hid[2, rows, :] = a
            au = a.astype(f32) * u
            dr_acc[rows, :] += au[:, :128] + au[:, 128:]

    def back(c, r):
        w = [wbuf[c, n].reshape(xs.shape[1], CHUNK) for n in range(3)]
        for m in range(r * ROWS, (r + 1) * ROWS, SUB):
            rows = pl.ds(m, SUB)
            dx_acc[rows, :] += dot(hid[0, rows, :], w[0], 1, 1) + dot(hid[1, rows, :], w[1], 1, 1)

    def weight_grads(c):
        for n, t in enumerate((xt, xt, gt)):
            dw[c, n] = dot(t[...], hid[n], 1, 0).reshape(dw.shape[2:])

    first_sends = [tcopy(3 * r + w, w, p, to, True) for r, to in ((0, xr), (1, xl), (2, partner)) for w in (2, 0, 1)]
    for c in first_sends:
        c.start()

    def own_piece(c, carry):
        for n, w in enumerate((w1_ref, w3_ref, w2_ref)):
            wbuf[c, n, z, y] = w[:, pl.ds(pl.multiple_of(c * CHUNK, CHUNK), CHUNK)]
        return carry
    lax.fori_loop(0, chunks, own_piece, 0)
    dr_acc[...] = jnp.zeros_like(dr_acc)
    dx_acc[...] = jnp.zeros_like(dx_acc)

    second = [tcopy(n, w, src, to) for n, w, src, to in
              ((18 + 2, 2, xl, xr), (18 + 1, 1, xl, xr), (18 + 0, 0, xr, xl))]
    forward_lr = [tcopy(3 * r + w, w, src, partner) for r, src in ((3, xl), (4, xr)) for w in (2, 0, 1)]
    forward_o = [tcopy(15 + w, w, xo, partner) for w in (2, 0, 1)]

    def back_block(which, q):
        return xs.at[pl.ds(pl.multiple_of(q * cap, cap), cap)] if which == 0 else dr_send.at[q]

    def xcopy(r, which, dst_peer, slot):
        return pltpu.make_async_remote_copy(
            src_ref=back_block(which, dst_peer), dst_ref=(dx_in, dr_in)[which].at[slot],
            send_sem=xsend.at[r, which], recv_sem=xrecv.at[r, which],
            device_id={"ep": dst_peer}, device_id_type=MESH)

    own = [pltpu.make_async_copy(back_block(n, p), d.at[p], loc_sem.at[n]) for n, d in enumerate((dx_in, dr_in))]
    sent = [[xcopy(r, w, peer[r], p) for r in range(PEERS - 1)] for w in (0, 1)]

    def tokens_1():
        arrived(2, partner)
        build_pair(chip, None, partner)

    def tokens_3():
        arrived(0, xl)
        arrived(1, xr)
        for c in second + forward_lr:
            c.start()

    def tokens_4():
        arrived(3, xpl)
        build_pair(left, xl, xpl)

    def tokens_5():
        arrived(4, xpr)
        build_pair(right, xr, xpr)
        arrived(6, xo)
        for c in forward_o:
            c.start()

    def tokens_6():
        arrived(5, xpo)
        build_pair(across, xo, xpo)

    def send_back():
        xs[...] = dx_acc[...].astype(bf16)
        for c in own[:1] + sent[0]:
            c.start()
        for e in range(PEERS):
            total = jnp.sum(dr_acc[e * cap:(e + 1) * cap, :], axis=1, keepdims=True)
            here = picked(meta_all[e, pl.ds(p, 1), :])
            dr_send[e, 0:1, :] = jnp.sum(jnp.where(here, total, 0.0), axis=0, keepdims=True)
        for c in own[1:] + sent[1]:
            c.start()

    def combine():
        for r in range(PEERS - 1):
            for w in (0, 1):
                xcopy(r, w, peer[r], lax.rem(p + PEERS - 1 - r, PEERS)).wait_recv()
        for c in own:
            c.wait()
        gx = jnp.zeros(gx_out.shape, f32)
        rw = [jnp.zeros((1, tokens), f32) for _ in (0, 1)]
        for e in range(PEERS):
            here = jnp.where(picked(meta_ref[e:e + 1, :]), 1.0, 0.0).astype(bf16)
            gx = gx + dot(here, dx_in[e], 0, 0)
            rw = [rw[j] + jnp.where(ids_ref[j:j + 1, :] == e, dr_in[e, 0:1, :], 0.0) for j in (0, 1)]
        gx_out[...] = gx.astype(bf16)
        for j in (0, 1):
            rw_out[j:j + 1, :] = rw[j]

    def compute(c, r):
        if r < tiles:
            forward(c, r)
        else:
            weight_grads(c)
        if r:
            back(c, r - 1)

    lead = HOPS + 1
    steps = lead + rounds * chunks

    def step(t, carry):
        n = t - lead
        c, r = lax.div(lax.max(n, 0), rounds), lax.rem(lax.max(n, 0), rounds)
        @pl.when(r == 0)
        def _():
            gather_round(lax.min(t, lead) + c)
        for j in range(rounds):
            @pl.when(jnp.logical_and(jnp.logical_and(n >= 0, t < steps), r == j))
            def _(j=j):
                for u in range(0 if j == 0 else SERVE[j - 1] + 1, SERVE[j] + 1):
                    compute(c, u)

        for at, event in ((1, tokens_1), (3, tokens_3), (4, tokens_4), (5, tokens_5), (6, tokens_6),
                          (steps, send_back), (steps + HOPS - 1, combine)):
            pl.when(t == at)(event)

        @pl.when(n >= 0)
        def _():
            serve(n + 1)
        return carry
    lax.fori_loop(0, steps + HOPS, step, 0)

    for c in first_sends + second + forward_lr + forward_o + sent[0] + sent[1]:
        c.wait_send()


def moe_step(x_tok, dy_tok, ids, route, w1, w3, w2t, capacity):
    tok_dev, d_model = x_tok.shape
    width = w1.shape[1]
    n_rows = PEERS * capacity
    block, chunks, half = d_model // RING, width // CHUNK, CHUNK // 2
    f32, bf16 = jnp.float32, jnp.bfloat16
    vmem = pl.BlockSpec(memory_space=pltpu.VMEM)
    hbm = pl.BlockSpec(memory_space=pl.ANY)
    dma = pltpu.SemaphoreType.DMA
    landing = jax.ShapeDtypeStruct((PEERS, tok_dev, d_model), bf16)
    grad = jax.ShapeDtypeStruct((3, block, width), f32)
    meta = jax.ShapeDtypeStruct((2 * PEERS, tok_dev), f32)
    return pl.pallas_call(
        moe_kernel,
        out_shape=(jax.ShapeDtypeStruct((tok_dev, d_model), bf16), jax.ShapeDtypeStruct(route.shape, f32),
                   grad, landing, landing),
        in_specs=[hbm, hbm] + [vmem] * 5,
        out_specs=[vmem] * 3 + [hbm, hbm],
        scratch_shapes=[
            pltpu.VMEM(meta.shape, f32),
            pltpu.VMEM((PEERS, *meta.shape), f32),
            pltpu.VMEM((PEERS, capacity, d_model), bf16),
            pltpu.VMEM((PEERS, 8, tok_dev), f32),
            pltpu.VMEM((2, 2, tok_dev, d_model), bf16),
            pltpu.VMEM((chunks, 3, NZ, NY, block, CHUNK), bf16),
            pltpu.VMEM((chunks, 3, NZ, NY, block, CHUNK), f32),
            pltpu.VMEM((SETS, 2, 3, NY // 2, block, half), f32),
            pltpu.VMEM((SETS, 2, 3, 3, NY, block, half), f32),
            pltpu.VMEM((SETS, 2, 3, 16, half), f32),
            pltpu.VMEM((SETS, 2, 3, block, half), f32),
            pltpu.VMEM((SETS, 2, 3, NZ // 2, block, half), f32),
            pltpu.VMEM((SETS, 2, 3, NZ, block, half), f32),
            pltpu.VMEM((SETS, 2, 3, 16, half), f32),
            pltpu.VMEM((SETS, 2, 3, 3, block, half), f32),
            pltpu.VMEM((n_rows, d_model), bf16),
            pltpu.VMEM((n_rows, d_model), bf16),
            pltpu.VMEM((n_rows, d_model), bf16),
            pltpu.VMEM((d_model, n_rows), bf16),
            pltpu.VMEM((d_model, n_rows), bf16),
            pltpu.VMEM((3, n_rows, CHUNK), bf16),
            pltpu.VMEM((n_rows, d_model), f32),
            pltpu.VMEM((n_rows, 128), f32),
            pltpu.VMEM((PEERS, 8, tok_dev), f32),
            dma((2, 2)), dma((2,)), dma((21,)), dma((21,)),
            dma((chunks, 2, 2)), dma((chunks, HOPS, 2, 2)),
            dma((PEERS - 1, 2)), dma((PEERS - 1, 2)),
            dma((chunks, 2, 2)), dma((chunks, HOPS, 2, 2)),
            pltpu.SemaphoreType.REGULAR((chunks - SETS,)),
        ],
        compiler_params=pltpu.CompilerParams(
            collective_id=0, has_side_effects=True, vmem_limit_bytes=67043328),
        name="moe_step",
    )(x_tok, dy_tok, ids, route, w1, w3, w2t)


def solution(mesh):
    tok_spec = P(("fsdp", "ep"), None)
    spec_in = P("ep", "fsdp", None)
    spec_out = P("ep", None, "fsdp")

    def per_device(x_tok, dy_tok, expert_ids, route_w, w_gate, w_up, w_down):
        tok_dev, top_k = expert_ids.shape
        capacity = capacity_of(tok_dev, top_k, PEERS)
        gx, rw, g, _, _ = moe_step(
            x_tok, dy_tok, expert_ids.T, route_w.T, w_gate[0], w_up[0], w_down[0].T, capacity)
        return gx, rw.T, g[0][None], g[1][None], g[2].T[None]

    return jax.shard_map(
        per_device, mesh=mesh,
        in_specs=(tok_spec, tok_spec, tok_spec, tok_spec, spec_in, spec_in, spec_out),
        out_specs=(tok_spec, tok_spec, spec_in, spec_in, spec_out),
        check_vma=False)
```
